256 devices in a mesh: grp: 4 (over y), dev: 64 (over x, z, core).
Axes of the slice: x: 4, y: 4, z: 8, core: 2. Of those that a mesh axis runs over, the one named last changes fastest.
Arguments:
- labels: int32 [256, 65536], P(('grp', 'dev')), may hold values from 0 to 16383, as said below
- present: int32 [256, 512], P(('grp', 'dev')), may hold values from 0 to 16383, as said below
- values: bfloat16 [256, 64, 65536], P(('grp', 'dev')), may hold values from -8 to 8
Outputs:
- zone_mean: float32 [64, 16384], P(None, 'dev')
The draws below stay inside these ranges and needn't reach their ends.
Inputs may be any that keep to these rules, and one draw needn't show every extreme that they name: `present`: each tile's 512 listed zones are distinct and ascending; at most 16 of them lie in one block of 256 consecutive zones, and in each group of 64 consecutive tiles one such block holds exactly 16 zones of every tile of the group. `labels`: every label of a tile is one of that tile's listed zones.
All inputs are finite; a program needn't handle non-finite values.
Results may differ from the reference program's by a relative error of at most 0.0003.
Values sent between devices are 32-bit elements; how exact they have to be, the bound alone decides.
A program may use at most 64 MiB of HBM per device.

```python
import jax
import jax.numpy as jnp
from jax import lax

ZONES = 16384
TIMES = 64
PIX_DEV = 65536
PRESENT = 512
RANGE = 256
CAP = 16
N_GRP = 4
N_DEV = 64


def layout_draw(key):
    tile_keys = jax.random.split(jax.random.fold_in(key, 11), N_GRP * N_DEV)
    group_keys = jax.random.split(jax.random.fold_in(key, 13), N_GRP)
    full_owner = jax.vmap(lambda single: jax.random.randint(single, (), 0, N_DEV))(group_keys)
    tile_full = jnp.repeat(full_owner, N_DEV)

    def one_tile(single, full):
        key_pick, key_offset, key_pixel = jax.random.split(single, 3)
        picked = jax.random.permutation(key_pick, (N_DEV - 1) * CAP)[:PRESENT - CAP]
        other_owner = picked // CAP
        slot_index = picked % CAP
        owner_index = jnp.where(other_owner >= full, other_owner + 1, other_owner)
        offset_table = jax.vmap(lambda part_key: jax.random.permutation(part_key, RANGE)[:CAP])(jax.random.split(key_offset, N_DEV))
        listed_ids = jnp.concatenate([owner_index * RANGE + offset_table[owner_index, slot_index], full * RANGE + offset_table[full]])
        listed_ids = jnp.sort(listed_ids).astype(jnp.int32)
        chosen = jax.random.randint(key_pixel, (PIX_DEV,), 0, PRESENT)
        return (listed_ids, listed_ids[chosen].astype(jnp.int32))
    return jax.vmap(one_tile)(tile_keys, tile_full)


def draw_present(key, part):
    return layout_draw(key)[0]


def draw_labels(key, part):
    return layout_draw(key)[1]


def draw_values(key, part):
    pixel_labels = layout_draw(key)[1]
    key_effect = jax.random.fold_in(key, 17)
    key_noise = jax.random.fold_in(key, 19)
    field_effect = jnp.clip(jax.random.normal(key_effect, (ZONES, TIMES), jnp.float32), -4.0, 4.0)

    def one_tile(item):
        tile_labels, single = item
        noise_part = jax.random.normal(single, (TIMES, PIX_DEV), jnp.float32)
        return jnp.clip(field_effect[tile_labels].T + noise_part, -8.0, 8.0).astype(jnp.bfloat16)
    return lax.map(one_tile, (pixel_labels, jax.random.split(key_noise, N_GRP * N_DEV)))


def setup_inputs(seed: int = 0) -> dict:
    arg_keys = jax.random.split(jax.random.key(seed), 4)
    labels = draw_labels(jax.random.fold_in(arg_keys[3], 71), 0)
    present = draw_present(jax.random.fold_in(arg_keys[3], 71), 0)
    values = draw_values(jax.random.fold_in(arg_keys[3], 71), 0)
    return {"labels": labels, "present": present, "values": values}


def reference(labels, present, values):
    def add_tile(carry, item):
        zone_totals, zone_counts = carry
        tile_labels, listed_ids, tile_values = item
        position = jnp.clip(jnp.searchsorted(listed_ids, tile_labels), 0, PRESENT - 1).astype(jnp.int32)
        counted = (listed_ids[position] == tile_labels).astype(jnp.float32)
        weighted = tile_values.astype(jnp.float32).T * counted[:, None]
        zone_totals = zone_totals + jax.ops.segment_sum(weighted, tile_labels, num_segments=ZONES)
        zone_counts = zone_counts + jax.ops.segment_sum(counted, tile_labels, num_segments=ZONES)
        return (zone_totals, zone_counts), None

    start = (jnp.zeros((ZONES, TIMES), jnp.float32), jnp.zeros((ZONES,), jnp.float32))
    (zone_totals, zone_counts), _ = lax.scan(add_tile, start, (labels, present, values))
    return (zone_totals / jnp.maximum(zone_counts, 1.0)[:, None]).T
```

```python
import functools

import jax
import jax.numpy as jnp
from jax import lax
from jax.experimental import pallas as pl
from jax.experimental.pallas import tpu as pltpu
from jax.sharding import PartitionSpec as P

ZONES = 16384
RANGE = 256
CAP = 16
CHUNKS = 8
F32, BF16, F8, I32 = jnp.float32, jnp.bfloat16, jnp.float8_e4m3fn, jnp.int32
MESH = pl.DeviceIdType.MESH
VMEM = pl.BlockSpec(memory_space=pltpu.VMEM)
ANY = pl.BlockSpec(memory_space=pl.ANY)
VMEM_ALL = 67043328


def nt(a, b):
    return lax.dot_general(a, b, (((1,), (1,)), ((), ())), preferred_element_type=F32)


def nn(a, b):
    return lax.dot_general(a, b, (((1,), (0,)), ((), ())), preferred_element_type=F32)


def onehot(mask, dtype=BF16):
    return jnp.where(mask, 1.0, 0.0).astype(dtype)


def two_parts(x):
    high = x.astype(BF16)
    return high, (x - high.astype(F32)).astype(BF16)


def lookup(table, word):
    row, lane = word >> 7, word & 127
    out = jnp.zeros_like(word)
    for a in range(8):
        source = jnp.broadcast_to(table[a : a + 1, :], word.shape)
        out = jnp.where(row == a, jnp.take_along_axis(source, lane, axis=1), out)
    return out


def table_kernel(present_ref, table_ref, slot_ref):
    present = present_ref[...]
    row8 = lax.broadcasted_iota(I32, (8, 128), 0)
    row128 = lax.broadcasted_iota(I32, (128, 128), 0)
    bitmap = jnp.zeros((8, 128), F32)
    prefix = jnp.zeros((8, 128), F32)
    ones = jnp.ones((128, 128), BF16)
    for c in range(4):
        zone = present[c : c + 1, :]
        top = jnp.broadcast_to(zone >> 11, (8, 128))
        middle = jnp.broadcast_to((zone >> 4) & 127, (128, 128))
        power = (jnp.full_like(zone, 1) << (zone & 15)).astype(F32)
        weight = jnp.where(top == row8, jnp.broadcast_to(power, (8, 128)), 0.0).astype(BF16)
        bitmap += nt(weight, onehot(middle == row128))
        prefix += nt(onehot(top == row8), onehot(middle < row128)) + nt(onehot(top < row8), ones)
    table = (prefix.astype(I32) << 16) | bitmap.astype(I32)
    table_ref[...] = table
    first = lookup(table, (present >> 8) << 4) >> 16
    place = lax.broadcasted_iota(I32, present.shape, 0) * 128 + lax.broadcasted_iota(I32, present.shape, 1)
    slot_ref[...] = place - first


def rank_of(labels, table):
    entry = lookup(table, labels >> 4)
    bit = labels & 15
    below = (jnp.full_like(bit, 1) << bit) - 1
    rank = (entry >> 16) + lax.population_count(entry & 65535 & below)
    listed = ((entry >> bit) & 1) == 1
    return rank & 255, jnp.where(listed, rank >> 8, 8)


def sums_kernel(table_ref, labels_ref, values_ref, out_ref, buf, lo_ref, hi_ref, sems):
    width = buf.shape[2]
    steps = width // 256

    def chunk_copy(k):
        return pltpu.make_async_copy(
            values_ref.at[:, pl.ds(pl.multiple_of(k * width, width), width)], buf.at[k], sems.at[k]
        )

    for k in range(CHUNKS):
        chunk_copy(k).start()
    table = table_ref[...]

    @pl.loop(0, lo_ref.shape[0] // 64)
    def _(i):
        rows = pl.ds(pl.multiple_of(i * 64, 64), 64)
        labels = labels_ref[rows, :]
        low, high = [], []
        for k in range(8):
            a, b = rank_of(labels[8 * k : 8 * k + 8], table)
            low.append(a)
            high.append(b)
        lo_ref[rows, :] = jnp.concatenate(low, 0).astype(F32)
        hi_ref[rows, :] = jnp.concatenate(high, 0).astype(F32)

    def run(*refs):
        accs = (refs[:3], refs[3:])
        for q in range(2):
            for a in accs[q]:
                pltpu.matmul_pop(a)
        row256 = lax.broadcasted_iota(I32, (256, 128), 0).astype(F32).astype(BF16)
        row16 = lax.broadcasted_iota(I32, (16, 128), 0).astype(F32).astype(BF16)
        one, zero = jnp.ones((), BF16), jnp.zeros((), BF16)

        @pl.loop(0, CHUNKS)
        def _(k):
            chunk_copy(k).wait()
            for j in range(steps):
                q, reg = j % 2, (j // 2) % 2
                hots, first, second, marks = [], [], [], []
                for s in range(2):
                    row = k * (width // 128) + 2 * j + s
                    low = jnp.broadcast_to(lo_ref[pl.ds(row, 1), :], (16, 128)).astype(BF16)
                    high = jnp.broadcast_to(hi_ref[pl.ds(row, 1), :], (16, 128)).astype(BF16)
                    hots.append(jnp.where(jnp.tile(low, (16, 1)) == row256, one, zero).astype(F8))
                    pixels = buf[k, :, pl.ds(256 * j + 128 * s, 128)]
                    high64 = jnp.tile(high, (4, 1))
                    first.append(jnp.where(high64 == zero, pixels, zero))
                    second.append(jnp.where(high64 == one, pixels, zero))
                    marks.append(jnp.where(high == row16, one, zero))
                joined = [jnp.concatenate(p, 1) for p in (hots, first, second, marks)]
                pltpu.matmul_push_rhs(joined[0], staging_register=reg, mxu_index=q, transpose=True)
                pltpu.matmul_acc_lhs(accs[q][0], joined[1], load_staged_rhs=reg)
                pltpu.matmul_acc_lhs(accs[q][1], joined[2])
                pltpu.matmul_acc_lhs(accs[q][2], joined[3])

        for a, b, at, rows in zip(accs[0], accs[1], (0, 64, 128), (64, 64, 16)):
            out_ref[at : at + rows, :] = pltpu.matmul_pop(a) + pltpu.matmul_pop(b)

    specs = []
    for q in range(2):
        specs += [pltpu.ACC(q)((rows, 256), F32) for rows in (64, 64, 16)]
    pl.run_scoped(run, *specs)


def pick_kernel(owners, present_ref, slot_ref, sums_ref, me_ref, tiles_ref, places_ref, counts_ref):
    present = present_ref[...]
    slot = slot_ref[...]
    total = jnp.zeros((owners * 8, 256), F32)
    places = jnp.zeros((owners, 128), F32)
    counts = jnp.zeros((owners, 128), F32)
    owner_row = lax.broadcasted_iota(I32, (owners, 256), 0)
    pair_row = lax.broadcasted_iota(I32, (owners * 8, 256), 0)
    lane_row = lax.broadcasted_iota(I32, (128, 256), 0)
    shift = (me_ref[0] & 7) * CAP
    empty = jnp.zeros((64, 256), BF16)
    for h in range(2):
        zone = jnp.concatenate([present[2 * h : 2 * h + 1], present[2 * h + 1 : 2 * h + 2]], 1)
        at = jnp.concatenate([slot[2 * h : 2 * h + 1], slot[2 * h + 1 : 2 * h + 2]], 1)
        owner = zone >> 8
        place = (owner << 3) + (at & 7)
        place_b = jnp.broadcast_to(place, (owners * 8, 256))
        parity_b = jnp.broadcast_to(at >> 3, (owners * 8, 256))
        high, rest = two_parts(sums_ref[64 * h : 64 * h + 64, :])
        for parity in range(2):
            pick = onehot((place_b == pair_row) & (parity_b == parity))
            order = (high, empty, rest, empty) if parity == 0 else (empty, high, empty, rest)
            total += nt(pick, jnp.concatenate(order, 0))
        mine = jnp.broadcast_to(owner, (owners, 256)) == owner_row
        lanes = onehot(jnp.broadcast_to(at, (128, 256)) + shift == lane_row)
        number = jnp.broadcast_to(((zone & 255) + 1).astype(F32), (owners, 256))
        places += nt(jnp.where(mine, number, 0.0).astype(BF16), lanes)
        for part in two_parts(sums_ref[128 + h : 129 + h, :]):
            spread = jnp.broadcast_to(part.astype(F32), (owners, 256))
            counts += nt(jnp.where(mine, spread, 0.0).astype(BF16), lanes)
    tiles_ref[...] = (total[:, :128] + total[:, 128:]).reshape(owners, 8, 128)
    places_ref[:, 0, :] = places
    counts_ref[:, 0, :] = counts


def exchange_kernel(
    owners, groups, tiles_ref, places_ref, counts_ref, out_ref,
    got_tiles, got_places, got_counts, ours, theirs, send_sems, recv_sems, y_send, y_recv,
):
    g, me = lax.axis_index("grp"), lax.axis_index("dev")
    barrier = pltpu.get_barrier_semaphore()

    @pl.loop(1, owners)
    def _(k):
        pl.semaphore_signal(barrier, inc=1, device_id=(g, lax.rem(me + k, owners)), device_id_type=MESH)

    @pl.loop(1, groups)
    def _(k):
        pl.semaphore_signal(barrier, inc=1, device_id=(lax.rem(g + k, groups), me), device_id_type=MESH)

    pl.semaphore_wait(barrier, owners + groups - 2)
    pairs = ((tiles_ref, got_tiles), (places_ref, got_places), (counts_ref, got_counts))

    @pl.loop(1, owners)
    def _(k):
        to = lax.rem(me + k, owners)
        for n, (source, landing) in enumerate(pairs):
            pltpu.make_async_remote_copy(
                src_ref=source.at[to], dst_ref=landing.at[me], send_sem=send_sems.at[n],
                recv_sem=recv_sems.at[n], device_id=(g, to), device_id_type=MESH,
            ).start()

    for source, landing in pairs:
        landing[me] = source[me]
    for n, (source, landing) in enumerate(pairs):
        whole = pltpu.make_async_remote_copy(
            src_ref=source.at[pl.ds(0, owners - 1)], dst_ref=landing.at[pl.ds(0, owners - 1)],
            send_sem=send_sems.at[n], recv_sem=recv_sems.at[n],
            device_id=(g, lax.rem(me + 1, owners)), device_id_type=MESH,
        )
        whole.wait_recv()
        whole.wait_send()

    place = jnp.sum(got_places[:, 0, :].reshape(owners // 8, 8, 128), axis=1)
    count = jnp.sum(got_counts[:, 0, :].reshape(owners // 8, 8, 128), axis=1)
    number = lax.broadcasted_iota(I32, (RANGE, 128), 0).astype(F32) + 1.0
    lane = lax.broadcasted_iota(I32, (8, 8, 128), 2)
    first_row = lax.broadcasted_iota(I32, (16, 128), 0)
    sums = jnp.zeros((RANGE, 256), F32)
    counted = jnp.zeros((16, RANGE), F32)
    for i in range(owners // 8):
        put = onehot(jnp.broadcast_to(place[i : i + 1], (RANGE, 128)) == number)
        tiles = got_tiles[8 * i : 8 * i + 8]
        split = jnp.stack([jnp.where(lane < 64, tiles, 0.0), jnp.where(lane < 64, 0.0, tiles)], 1)
        sums += nn(put, jnp.concatenate(two_parts(split.reshape(128, 128)), 1))
        high, rest = (jnp.broadcast_to(p.astype(F32), (16, 128)) for p in two_parts(count[i : i + 1]))
        marks = jnp.where(first_row == 0, high, jnp.where(first_row == 1, rest, 0.0))
        counted += nt(marks.astype(BF16), put)
    both = (sums[:, :128] + sums[:, 128:]).T
    ours[0:64] = both[:64] + both[64:]
    ours[64:72] = jnp.broadcast_to(counted[0:1] + counted[1:2], (8, RANGE))

    @pl.loop(1, groups)
    def _(k):
        to = lax.rem(g + k, groups)
        pltpu.make_async_remote_copy(
            src_ref=ours, dst_ref=theirs.at[k - 1], send_sem=y_send.at[k - 1], recv_sem=y_recv.at[k - 1],
            device_id=(to, me), device_id_type=MESH,
        ).start()

    total = ours[...]
    for k in range(1, groups):
        copy = pltpu.make_async_remote_copy(
            src_ref=ours, dst_ref=theirs.at[k - 1], send_sem=y_send.at[k - 1], recv_sem=y_recv.at[k - 1],
            device_id=(lax.rem(g + k, groups), me), device_id_type=MESH,
        )
        copy.wait_recv()
        total = total + theirs[k - 1]
    for k in range(1, groups):
        pltpu.make_async_remote_copy(
            src_ref=ours, dst_ref=theirs.at[k - 1], send_sem=y_send.at[k - 1], recv_sem=y_recv.at[k - 1],
            device_id=(lax.rem(g + k, groups), me), device_id_type=MESH,
        ).wait_send()
    out_ref[...] = total


def shaped(shape, dtype=F32):
    return jax.ShapeDtypeStruct(shape, dtype)


def local_sums(table, labels, values):
    times, pixels = values.shape
    return pl.pallas_call(
        sums_kernel,
        out_shape=shaped((144, 256)),
        in_specs=[VMEM, VMEM, ANY],
        out_specs=VMEM,
        scratch_shapes=[
            pltpu.VMEM((CHUNKS, times, pixels // CHUNKS), BF16),
            pltpu.VMEM((pixels // 128, 128), F32),
            pltpu.VMEM((pixels // 128, 128), F32),
            pltpu.SemaphoreType.DMA((CHUNKS,)),
        ],
        compiler_params=pltpu.CompilerParams(vmem_limit_bytes=VMEM_ALL),
    )(table, labels.reshape(pixels // 128, 128), values)


def exchange(owners, groups, tiles, places, counts):
    return pl.pallas_call(
        functools.partial(exchange_kernel, owners, groups),
        out_shape=shaped((72, RANGE)),
        in_specs=[VMEM, VMEM, VMEM],
        out_specs=VMEM,
        scratch_shapes=[
            pltpu.VMEM((owners, 8, 128), F32),
            pltpu.VMEM((owners, 1, 128), F32),
            pltpu.VMEM((owners, 1, 128), F32),
            pltpu.VMEM((72, RANGE), F32),
            pltpu.VMEM((groups - 1, 72, RANGE), F32),
            pltpu.SemaphoreType.DMA((3,)),
            pltpu.SemaphoreType.DMA((3,)),
            pltpu.SemaphoreType.DMA((groups - 1,)),
            pltpu.SemaphoreType.DMA((groups - 1,)),
        ],
        compiler_params=pltpu.CompilerParams(collective_id=0, has_side_effects=True),
    )(tiles, places, counts)


def body(labels, present, values):
    owners, groups = lax.axis_size("dev"), lax.axis_size("grp")
    listed = present.reshape(4, 128)
    table, slot = pl.pallas_call(
        table_kernel, out_shape=(shaped((8, 128), I32), shaped((4, 128), I32)),
        in_specs=[VMEM], out_specs=(VMEM, VMEM),
    )(listed)
    sums = local_sums(table, labels, values[0])
    me = lax.axis_index("dev").astype(I32).reshape(1)
    tiles, places, counts = pl.pallas_call(
        functools.partial(pick_kernel, owners),
        out_shape=(shaped((owners, 8, 128)), shaped((owners, 1, 128)), shaped((owners, 1, 128))),
        in_specs=[VMEM, VMEM, VMEM, pl.BlockSpec(memory_space=pltpu.SMEM)],
        out_specs=(VMEM, VMEM, VMEM),
    )(listed, slot, sums, me)
    total = exchange(owners, groups, tiles, places, counts)
    return total[:64] / jnp.maximum(total[64:65], 1.0)


def solution(mesh):
    return jax.shard_map(
        body,
        mesh=mesh,
        in_specs=(P(("grp", "dev"), None), P(("grp", "dev"), None), P(("grp", "dev"), None, None)),
        out_specs=P(None, "dev"),
        check_vma=False,
    )
```

```python
import functools

import jax
import jax.numpy as jnp
from jax import lax
from jax.experimental import pallas as pl
from jax.experimental.pallas import tpu as pltpu
from jax.sharding import PartitionSpec as P

ZONES = 16384
RANGE = 256
CAP = 16
CHUNKS = 8
F32, BF16, F8, I32 = jnp.float32, jnp.bfloat16, jnp.float8_e4m3fn, jnp.int32
MESH = pl.DeviceIdType.MESH
VMEM = pl.BlockSpec(memory_space=pltpu.VMEM)
ANY = pl.BlockSpec(memory_space=pl.ANY)
VMEM_ALL = 67043328


def onehot(mask, dtype=BF16):
    return jnp.where(mask, 1.0, 0.0).astype(dtype)


def two_parts(x):
    high = x.astype(BF16)
    return high, (x - high.astype(F32)).astype(BF16)


def lookup(table, word):
    row, lane = word >> 7, word & 127
    out = jnp.zeros_like(word)
    for a in range(8):
        source = jnp.broadcast_to(table[a : a + 1, :], word.shape)
        out = jnp.where(row == a, jnp.take_along_axis(source, lane, axis=1), out)
    return out


def rank_of(labels, table):
    entry = lookup(table, labels >> 4)
    bit = labels & 15
    below = (jnp.full_like(bit, 1) << bit) - 1
    rank = (entry >> 16) + lax.population_count(entry & 65535 & below)
    listed = ((entry >> bit) & 1) == 1
    return rank & 255, jnp.where(listed, rank >> 8, 8)


def wide(row, rows):
    return jnp.broadcast_to(row, (rows, row.shape[1]))


def beside(ref_value, h):
    return jnp.concatenate([ref_value[2 * h : 2 * h + 1], ref_value[2 * h + 1 : 2 * h + 2]], 1)


def make_table(present, accs):
    row8 = lax.broadcasted_iota(I32, (8, 256), 0)
    row128 = lax.broadcasted_iota(I32, (128, 256), 0)
    below = jnp.zeros((8, 1), F32)
    for h in range(2):
        zone = beside(present, h)
        top = wide(zone >> 11, 8)
        middle = wide((zone >> 4) & 127, 128)
        power = (jnp.full_like(zone, 1) << (zone & 15)).astype(F32)
        left = jnp.concatenate(
            [jnp.where(top == row8, wide(power, 8), 0.0), jnp.where(top == row8, 1.0, 0.0)], 0
        ).astype(BF16)
        right = jnp.concatenate([onehot(middle == row128), onehot(middle < row128)], 0)
        pltpu.matmul_push_rhs(right, staging_register=0, mxu_index=h, transpose=True)
        pltpu.matmul_acc_lhs(accs[h], left, load_staged_rhs=0)
        below += jnp.sum(jnp.where(top < row8, 1.0, 0.0), axis=1, keepdims=True)
    both = pltpu.matmul_pop(accs[0]) + pltpu.matmul_pop(accs[1])
    prefix = both[8:16, 128:256] + below
    return (prefix.astype(I32) << 16) | both[0:8, 0:128].astype(I32)


def fused_kernel(
    owners, groups, present_ref, labels_ref, values_ref, out_ref,
    buf, lab_ref, lo_ref, hi_ref, slot_ref, sums_ref, tiles_ref, places_ref, counts_ref,
    got_tiles, got_places, got_counts, ours, theirs,
    in_sems, lab_sem, send_sems, recv_sems, y_send, y_recv,
):
    g, me = lax.axis_index("grp"), lax.axis_index("dev")
    width = buf.shape[2]
    steps = width // 256
    one, zero = jnp.ones((), BF16), jnp.zeros((), BF16)

    def chunk_copy(k):
        return pltpu.make_async_copy(
            values_ref.at[:, pl.ds(pl.multiple_of(k * width, width), width)], buf.at[k], in_sems.at[k]
        )

    lab_copy = pltpu.make_async_copy(labels_ref, lab_ref, lab_sem)
    lab_copy.start()
    for k in range(CHUNKS):
        chunk_copy(k).start()

    barrier = pltpu.get_barrier_semaphore()

    @pl.loop(1, owners)
    def _(k):
        pl.semaphore_signal(barrier, inc=1, device_id=(g, lax.rem(me + k, owners)), device_id_type=MESH)

    @pl.loop(1, groups)
    def _(k):
        pl.semaphore_signal(barrier, inc=1, device_id=(lax.rem(g + k, groups), me), device_id_type=MESH)

    present = present_ref[...]
    owner_row = lax.broadcasted_iota(I32, (owners, 256), 0)
    lane_row = lax.broadcasted_iota(I32, (256, 256), 0)
    shift = (me & 7) * CAP

    def clear(*accs):
        for a in accs:
            pltpu.matmul_pop(a)

    pl.run_scoped(clear, *[pltpu.ACC(q)((1024, 256), F32) for q in range(2)])

    def prepare(*accs):
        table = make_table(present, accs[:2])
        first = lookup(table, (present >> 8) << 4) >> 16
        index = lax.broadcasted_iota(I32, present.shape, 0) * 128 + lax.broadcasted_iota(I32, present.shape, 1)
        slot = index - first
        for h in range(2):
            zone, at = beside(present, h), beside(slot, h)
            mine = wide(zone >> 8, owners) == owner_row
            lanes = onehot(wide(at, 256) + shift == lane_row)
            number = wide(((zone & 255) + 1).astype(F32), owners)
            pltpu.matmul_push_rhs(lanes, staging_register=0, mxu_index=h, transpose=True)
            pltpu.matmul_acc_lhs(accs[2 + h], jnp.where(mine, number, 0.0).astype(BF16), load_staged_rhs=0)
        places_ref[:, 0, :] = (pltpu.matmul_pop(accs[2]) + pltpu.matmul_pop(accs[3]))[:, :128]
        lab_copy.wait()

        @pl.loop(0, lo_ref.shape[0] // 64)
        def _(i):
            rows = pl.ds(pl.multiple_of(i * 64, 64), 64)
            labels = lab_ref[rows, :]
            low, high = [], []
            for k in range(8):
                a, b = rank_of(labels[8 * k : 8 * k + 8], table)
                low.append(a)
                high.append(b)
            lo_ref[rows, :] = jnp.concatenate(low, 0).astype(F32)
            hi_ref[rows, :] = jnp.concatenate(high, 0).astype(F32)

        slot_ref[...] = slot

    pl.run_scoped(prepare, *[pltpu.ACC(q)((rows, 256), F32) for rows in (16, owners) for q in range(2)])

    def send(n, source, landing, k):
        to = lax.rem(me + k, owners)
        pltpu.make_async_remote_copy(
            src_ref=source.at[to], dst_ref=landing.at[me], send_sem=send_sems.at[n],
            recv_sem=recv_sems.at[n], device_id=(g, to), device_id_type=MESH,
        ).start()

    def add_up(*refs):
        accs = (refs[:3], refs[3:])
        row256 = lax.broadcasted_iota(I32, (256, 128), 0).astype(F32).astype(BF16)
        row16 = lax.broadcasted_iota(I32, (16, 128), 0).astype(F32).astype(BF16)

        def chunk(k):
            chunk_copy(k).wait()
            for j in range(steps):
                q, reg = j % 2, (j // 2) % 2
                hots, first, second, marks = [], [], [], []
                for s in range(2):
                    row = k * (width // 128) + 2 * j + s
                    low = wide(lo_ref[pl.ds(row, 1), :], 16).astype(BF16)
                    high = wide(hi_ref[pl.ds(row, 1), :], 16).astype(BF16)
                    hots.append(jnp.where(jnp.tile(low, (16, 1)) == row256, one, zero).astype(F8))
                    pixels = buf[k, :, pl.ds(256 * j + 128 * s, 128)]
                    high64 = jnp.tile(high, (4, 1))
                    first.append(jnp.where(high64 == zero, pixels, zero))
                    second.append(jnp.where(high64 == one, pixels, zero))
                    marks.append(jnp.where(high == row16, one, zero))
                joined = [jnp.concatenate(p, 1) for p in (hots, first, second, marks)]
                pltpu.matmul_push_rhs(joined[0], staging_register=reg, mxu_index=q, transpose=True)
                pltpu.matmul_acc_lhs(accs[q][0], joined[1], load_staged_rhs=reg)
                pltpu.matmul_acc_lhs(accs[q][1], joined[2])
                pltpu.matmul_acc_lhs(accs[q][2], joined[3])

        pl.loop(0, CHUNKS - 2)(chunk)
        pl.semaphore_wait(barrier, owners + groups - 2)
        pl.loop(1, owners)(functools.partial(send, 0, places_ref, got_places))
        pl.loop(CHUNKS - 2, CHUNKS)(chunk)
        for a, b, at, rows in zip(accs[0], accs[1], (0, 64, 128), (64, 64, 16)):
            sums_ref[at : at + rows, :] = pltpu.matmul_pop(a) + pltpu.matmul_pop(b)

    pl.run_scoped(add_up, *[pltpu.ACC(q)((rows, 256), F32) for q in range(2) for rows in (64, 64, 16)])

    def pick_slots(*accs):
        slot = slot_ref[...]
        pair_row = lax.broadcasted_iota(I32, (owners * 8, 256), 0)
        empty = jnp.zeros((64, 256), BF16)
        for h in range(2):
            zone, at = beside(present, h), beside(slot, h)
            owner = zone >> 8
            target = ((owner << 3) + (at & 7)) * 2 + (at >> 3)
            high, rest = two_parts(sums_ref[64 * h : 64 * h + 64, :])
            for parity in range(2):
                order = (high, empty, rest, empty) if parity == 0 else (empty, high, empty, rest)
                pltpu.matmul_push_rhs(
                    jnp.concatenate(order, 0), staging_register=h, mxu_index=parity, transpose=True
                )
                pick = onehot(wide(target, owners * 8) == pair_row * 2 + parity)
                pltpu.matmul_acc_lhs(accs[parity], pick, load_staged_rhs=h)
            mine = wide(owner, owners) == owner_row
            lanes = onehot(wide(at, 256) + shift == lane_row)
            parts = [
                jnp.where(mine, wide(part.astype(F32), owners), 0.0)
                for part in two_parts(sums_ref[128 + h : 129 + h, :])
            ]
            pltpu.matmul_push_rhs(lanes, staging_register=1 - h, mxu_index=h, transpose=True)
            pltpu.matmul_acc_lhs(accs[2 + h], jnp.concatenate(parts, 0).astype(BF16), load_staged_rhs=1 - h)
        total = pltpu.matmul_pop(accs[0]) + pltpu.matmul_pop(accs[1])
        counts = pltpu.matmul_pop(accs[2]) + pltpu.matmul_pop(accs[3])
        tiles_ref[...] = (total[:, :128] + total[:, 128:]).reshape(owners, 8, 128)
        counts_ref[:, 0, :] = counts[:owners, :128] + counts[owners:, :128]

    pl.run_scoped(pick_slots, *[pltpu.ACC(q)((rows, 256), F32) for rows in (owners * 8, owners * 2) for q in range(2)])

    pairs = ((places_ref, got_places), (tiles_ref, got_tiles), (counts_ref, got_counts))

    @pl.loop(1, owners)
    def _(k):
        for n in (1, 2):
            send(n, *pairs[n], k)

    for source, landing in pairs:
        landing[me] = source[me]
    for n, (source, landing) in enumerate(pairs):
        whole = pltpu.make_async_remote_copy(
            src_ref=source.at[pl.ds(0, owners - 1)], dst_ref=landing.at[pl.ds(0, owners - 1)],
            send_sem=send_sems.at[n], recv_sem=recv_sems.at[n],
            device_id=(g, lax.rem(me + 1, owners)), device_id_type=MESH,
        )
        whole.wait_recv()
        whole.wait_send()

    def place_slots(*accs):
        place = jnp.sum(got_places[:, 0, :].reshape(owners // 8, 8, 128), axis=1)
        count = jnp.sum(got_counts[:, 0, :].reshape(owners // 8, 8, 128), axis=1)
        number = lax.broadcasted_iota(I32, (RANGE, 256), 0).astype(F32) + 1.0
        lane = lax.broadcasted_iota(I32, (16, 8, 128), 2)
        row16 = lax.broadcasted_iota(I32, (16, 256), 0)
        for i in range(owners // 16):
            q = i % 2
            put = onehot(wide(beside(place, i), RANGE) == number)
            tiles = got_tiles[16 * i : 16 * i + 16]
            split = jnp.stack([jnp.where(lane < 64, tiles, 0.0), jnp.where(lane < 64, 0.0, tiles)], 1)
            right = jnp.concatenate(two_parts(split.reshape(256, 128)), 1)
            pltpu.matmul_push_rhs(right, staging_register=0, mxu_index=q)
            pltpu.matmul_acc_lhs(accs[q], put, load_staged_rhs=0)
            high, rest = (wide(p.astype(F32), 16) for p in two_parts(beside(count, i)))
            marks = jnp.where(row16 == 0, high, jnp.where(row16 == 1, rest, 0.0)).astype(BF16)
            pltpu.matmul_push_rhs(put, staging_register=1, mxu_index=q, transpose=True)
            pltpu.matmul_acc_lhs(accs[2 + q], marks, load_staged_rhs=1)
        sums = pltpu.matmul_pop(accs[0]) + pltpu.matmul_pop(accs[1])
        counted = pltpu.matmul_pop(accs[2]) + pltpu.matmul_pop(accs[3])
        both = (sums[:, :128] + sums[:, 128:]).T
        ours[0:64] = both[:64] + both[64:]
        ours[64:72] = wide(counted[0:1] + counted[1:2], 8)

    pl.run_scoped(place_slots, *[pltpu.ACC(q)((rows, 256), F32) for rows in (RANGE, 16) for q in range(2)])

    def y_copy(k):
        return pltpu.make_async_remote_copy(
            src_ref=ours, dst_ref=theirs.at[k - 1], send_sem=y_send.at[k - 1], recv_sem=y_recv.at[k - 1],
            device_id=(lax.rem(g + k, groups), me), device_id_type=MESH,
        )

    for k in range(1, groups):
        y_copy(k).start()
    total = ours[...]
    for k in range(1, groups):
        y_copy(k).wait_recv()
        total = total + theirs[k - 1]
    out_ref[...] = total[0:64] / jnp.maximum(total[64:65], 1.0)
    for k in range(1, groups):
        y_copy(k).wait_send()


def body(labels, present, values):
    owners, groups = lax.axis_size("dev"), lax.axis_size("grp")
    times, pixels = values.shape[1:]
    lines = pixels // 128
    return pl.pallas_call(
        functools.partial(fused_kernel, owners, groups),
        out_shape=jax.ShapeDtypeStruct((times, RANGE), F32),
        in_specs=[VMEM, ANY, ANY],
        out_specs=VMEM,
        scratch_shapes=[
            pltpu.VMEM((CHUNKS, times, pixels // CHUNKS), BF16),
            pltpu.VMEM((lines, 128), I32),
            pltpu.VMEM((lines, 128), F32),
            pltpu.VMEM((lines, 128), F32),
            pltpu.VMEM((4, 128), I32),
            pltpu.VMEM((144, 256), F32),
            pltpu.VMEM((owners, 8, 128), F32),
            pltpu.VMEM((owners, 1, 128), F32),
            pltpu.VMEM((owners, 1, 128), F32),
            pltpu.VMEM((owners, 8, 128), F32),
            pltpu.VMEM((owners, 1, 128), F32),
            pltpu.VMEM((owners, 1, 128), F32),
            pltpu.VMEM((72, RANGE), F32),
            pltpu.VMEM((groups - 1, 72, RANGE), F32),
            pltpu.SemaphoreType.DMA((CHUNKS,)),
            pltpu.SemaphoreType.DMA,
            pltpu.SemaphoreType.DMA((3,)),
            pltpu.SemaphoreType.DMA((3,)),
            pltpu.SemaphoreType.DMA((groups - 1,)),
            pltpu.SemaphoreType.DMA((groups - 1,)),
        ],
        compiler_params=pltpu.CompilerParams(
            collective_id=0, has_side_effects=True, vmem_limit_bytes=VMEM_ALL
        ),
    )(present.reshape(4, 128), labels.reshape(lines, 128), values[0])


def solution(mesh):
    return jax.shard_map(
        body,
        mesh=mesh,
        in_specs=(P(("grp", "dev"), None), P(("grp", "dev"), None), P(("grp", "dev"), None, None)),
        out_specs=P(None, "dev"),
        check_vma=False,
    )
```

```python
import functools

import jax
import jax.numpy as jnp
from jax import lax
from jax.experimental import pallas as pl
from jax.experimental.pallas import tpu as pltpu
from jax.sharding import PartitionSpec as P

ZONES = 16384
RANGE = 256
CAP = 16
CHUNKS = 8
F32, BF16, F8, I32 = jnp.float32, jnp.bfloat16, jnp.float8_e4m3fn, jnp.int32
MESH = pl.DeviceIdType.MESH
VMEM = pl.BlockSpec(memory_space=pltpu.VMEM)
ANY = pl.BlockSpec(memory_space=pl.ANY)
VMEM_LIMIT = 48 * 1024 * 1024


def onehot(mask, dtype=BF16):
    return jnp.where(mask, 1.0, 0.0).astype(dtype)


def two_parts(x):
    high = x.astype(BF16)
    return high, (x - high.astype(F32)).astype(BF16)


def lookup(table, word):
    row, lane = word >> 7, word & 127
    out = jnp.zeros_like(word)
    for a in range(8):
        source = jnp.broadcast_to(table[a : a + 1, :], word.shape)
        out = jnp.where(row == a, jnp.take_along_axis(source, lane, axis=1), out)
    return out


def rank_of(labels, table):
    entry = lookup(table, labels >> 4)
    bit = labels & 15
    below = (jnp.full_like(bit, 1) << bit) - 1
    rank = (entry >> 16) + lax.population_count(entry & 65535 & below)
    listed = ((entry >> bit) & 1) == 1
    return rank & 255, jnp.where(listed, rank >> 8, 8)


def wide(row, rows):
    return jnp.broadcast_to(row, (rows, row.shape[1]))


def beside(ref_value, h):
    return jnp.concatenate([ref_value[2 * h : 2 * h + 1], ref_value[2 * h + 1 : 2 * h + 2]], 1)


def make_table(present, accs):
    row8 = lax.broadcasted_iota(I32, (8, 256), 0)
    row128 = lax.broadcasted_iota(I32, (128, 256), 0)
    below = jnp.zeros((8, 1), F32)
    for h in range(2):
        zone = beside(present, h)
        top = wide(zone >> 11, 8)
        middle = wide((zone >> 4) & 127, 128)
        power = (jnp.full_like(zone, 1) << (zone & 15)).astype(F32)
        left = jnp.concatenate(
            [jnp.where(top == row8, wide(power, 8), 0.0), jnp.where(top == row8, 1.0, 0.0)], 0
        ).astype(BF16)
        right = jnp.concatenate([onehot(middle == row128), onehot(middle < row128)], 0)
        pltpu.matmul_push_rhs(right, staging_register=0, mxu_index=h, transpose=True)
        pltpu.matmul_acc_lhs(accs[h], left, load_staged_rhs=0)
        below += jnp.sum(jnp.where(top < row8, 1.0, 0.0), axis=1, keepdims=True)
    both = pltpu.matmul_pop(accs[0]) + pltpu.matmul_pop(accs[1])
    prefix = both[8:16, 128:256] + below
    return (prefix.astype(I32) << 16) | both[0:8, 0:128].astype(I32)


def fused_kernel(
    owners, listed_ref, labels_ref, values_ref, out_ref,
    buf, present_ref, lab_ref, lo_ref, hi_ref, table_ref, slot_ref, sums_ref, tiles_ref, places_ref, counts_ref,
    got_tiles, got_places, got_counts, put_ref, ours, partial, theirs,
    in_sems, listed_sem, lab_sem, send_sems, recv_sems, y_send, y_recv,
):
    g, me = lax.axis_index("grp"), lax.axis_index("dev")
    width = buf.shape[2]
    steps = width // 256
    one, zero = jnp.ones((), BF16), jnp.zeros((), BF16)

    def chunk_copy(k):
        return pltpu.make_async_copy(
            values_ref.at[:, pl.ds(pl.multiple_of(k * width, width), width)], buf.at[k], in_sems.at[k]
        )

    listed_copy = pltpu.make_async_copy(listed_ref, present_ref, listed_sem)
    listed_copy.start()
    lab_copy = pltpu.make_async_copy(labels_ref, lab_ref, lab_sem)
    lab_copy.start()
    barrier = pltpu.get_barrier_semaphore()

    beside_g = (g + 1 - 2 * lax.rem(g, 2), 3 - g)
    for k in range(1, owners):
        if k == 8:
            for n in range(CHUNKS):
                chunk_copy(n).start()
        pl.semaphore_signal(barrier, inc=1, device_id=(g, lax.rem(me + k, owners)), device_id_type=MESH)
    for other in beside_g:
        pl.semaphore_signal(barrier, inc=1, device_id=(other, me), device_id_type=MESH)

    listed_copy.wait()
    present = present_ref[...]
    owner_row = lax.broadcasted_iota(I32, (owners, 256), 0)
    lane_row = lax.broadcasted_iota(I32, (256, 256), 0)
    shift = (me & 7) * CAP

    def rank_chunk(k):
        rows = pl.ds(pl.multiple_of(k * 64, 64), 64)
        labels = lab_ref[rows, :]
        ranked = [rank_of(labels[8 * i : 8 * i + 8], table_ref[...]) for i in range(8)]
        lo_ref[rows, :] = jnp.concatenate([a for a, _ in ranked], 0).astype(F32)
        hi_ref[rows, :] = jnp.concatenate([b for _, b in ranked], 0).astype(F32)

    def prepare(*accs):
        table = make_table(present, accs[:2])
        first = lookup(table, (present >> 8) << 4) >> 16
        index = lax.broadcasted_iota(I32, present.shape, 0) * 128 + lax.broadcasted_iota(I32, present.shape, 1)
        slot = index - first
        for h in range(2):
            zone, at = beside(present, h), beside(slot, h)
            mine = wide(zone >> 8, owners) == owner_row
            lanes = onehot(wide(at, 256) + shift == lane_row)
            number = wide(((zone & 255) + 1).astype(F32), owners)
            pltpu.matmul_push_rhs(lanes, staging_register=0, mxu_index=h, transpose=True)
            pltpu.matmul_acc_lhs(accs[2 + h], jnp.where(mine, number, 0.0).astype(BF16), load_staged_rhs=0)
        places_ref[:, 0, :] = (pltpu.matmul_pop(accs[2]) + pltpu.matmul_pop(accs[3]))[:, :128]
        slot_ref[...] = slot
        table_ref[...] = table
        lab_copy.wait()
        rank_chunk(0)

    pl.run_scoped(prepare, *[pltpu.ACC(q)((rows, 256), F32) for rows in (16, owners) for q in range(2)])

    def send(n, source, landing, k):
        to = lax.rem(me + k, owners)
        pltpu.make_async_remote_copy(
            src_ref=source.at[to], dst_ref=landing.at[me], send_sem=send_sems.at[n],
            recv_sem=recv_sems.at[n], device_id=(g, to), device_id_type=MESH,
        ).start()

    def add_up(*refs):
        accs = (refs[:3], refs[3:])
        row256 = lax.broadcasted_iota(I32, (256, 128), 0).astype(F32).astype(BF16)
        row16 = lax.broadcasted_iota(I32, (16, 128), 0).astype(F32).astype(BF16)

        def chunk(k, beside_it=lambda: None):
            chunk_copy(k).wait()
            beside_it()
            for j in range(steps):
                q, reg = j % 2, (j // 2) % 2
                hots, first, second, marks = [], [], [], []
                for s in range(2):
                    row = k * (width // 128) + 2 * j + s
                    low = wide(lo_ref[pl.ds(row, 1), :], 16).astype(BF16)
                    high = wide(hi_ref[pl.ds(row, 1), :], 16).astype(BF16)
                    hots.append(jnp.where(jnp.tile(low, (16, 1)) == row256, one, zero).astype(F8))
                    pixels = buf[k, :, pl.ds(256 * j + 128 * s, 128)]
                    high64 = jnp.tile(high, (4, 1))
                    first.append(jnp.where(high64 == zero, pixels, zero))
                    second.append(jnp.where(high64 == one, pixels, zero))
                    marks.append(jnp.where(high == row16, one, zero))
                joined = [jnp.concatenate(p, 1) for p in (hots, first, second, marks)]
                pltpu.matmul_push_rhs(joined[0], staging_register=reg, mxu_index=q, transpose=True)
                pltpu.matmul_acc_lhs(accs[q][0], joined[1], load_staged_rhs=reg)
                pltpu.matmul_acc_lhs(accs[q][1], joined[2])
                pltpu.matmul_acc_lhs(accs[q][2], joined[3])

        @pl.loop(0, CHUNKS - 1)
        def _(k):
            chunk(k)
            rank_chunk(k + 1)

        pl.semaphore_wait(barrier, owners + 1)

        def send_places():
            for k in range(1, owners):
                send(0, places_ref, got_places, k)

        chunk(CHUNKS - 1, send_places)
        for a, b, at, rows in zip(accs[0], accs[1], (0, 64, 128), (64, 64, 16)):
            sums_ref[at : at + rows, :] = pltpu.matmul_pop(a) + pltpu.matmul_pop(b)

    pl.run_scoped(add_up, *[pltpu.ACC(q)((rows, 256), F32) for q in range(2) for rows in (64, 64, 16)])

    def pick_slots(*accs):
        slot = slot_ref[...]
        pair_row = lax.broadcasted_iota(I32, (owners * 8, 256), 0)
        empty = jnp.zeros((64, 256), BF16)
        for h in range(2):
            zone, at = beside(present, h), beside(slot, h)
            owner = zone >> 8
            target = ((owner << 3) + (at & 7)) * 2 + (at >> 3)
            high, rest = two_parts(sums_ref[64 * h : 64 * h + 64, :])
            for parity in range(2):
                order = (high, empty, rest, empty) if parity == 0 else (empty, high, empty, rest)
                pltpu.matmul_push_rhs(
                    jnp.concatenate(order, 0), staging_register=h, mxu_index=parity, transpose=True
                )
                pick = onehot(wide(target, owners * 8) == pair_row * 2 + parity)
                pltpu.matmul_acc_lhs(accs[parity], pick, load_staged_rhs=h)
            mine = wide(owner, owners) == owner_row
            lanes = onehot(wide(at, 256) + shift == lane_row)
            parts = [
                jnp.where(mine, wide(part.astype(F32), owners), 0.0)
                for part in two_parts(sums_ref[128 + h : 129 + h, :])
            ]
            pltpu.matmul_push_rhs(lanes, staging_register=1 - h, mxu_index=h, transpose=True)
            pltpu.matmul_acc_lhs(accs[2 + h], jnp.concatenate(parts, 0).astype(BF16), load_staged_rhs=1 - h)
        total = pltpu.matmul_pop(accs[0]) + pltpu.matmul_pop(accs[1])
        counts = pltpu.matmul_pop(accs[2]) + pltpu.matmul_pop(accs[3])
        tiles_ref[...] = (total[:, :128] + total[:, 128:]).reshape(owners, 8, 128)
        counts_ref[:, 0, :] = counts[:owners, :128] + counts[owners:, :128]

    pl.run_scoped(pick_slots, *[pltpu.ACC(q)((rows, 256), F32) for rows in (owners * 8, owners * 2) for q in range(2)])

    pairs = ((places_ref, got_places), (tiles_ref, got_tiles), (counts_ref, got_counts))

    @pl.loop(0, owners // 9)
    def _(i):
        for k in range(9):
            for n in (1, 2):
                send(n, *pairs[n], i * 9 + k + 1)

    for source, landing in pairs:
        landing[me] = source[me]

    def arrived(n):
        source, landing = pairs[n]
        whole = pltpu.make_async_remote_copy(
            src_ref=source.at[pl.ds(0, owners - 1)], dst_ref=landing.at[pl.ds(0, owners - 1)],
            send_sem=send_sems.at[n], recv_sem=recv_sems.at[n],
            device_id=(g, lax.rem(me + 1, owners)), device_id_type=MESH,
        )
        whole.wait_recv()
        whole.wait_send()

    arrived(0)
    place = jnp.sum(got_places[:, 0, :].reshape(owners // 8, 8, 128), axis=1)
    number = lax.broadcasted_iota(I32, (RANGE, 256), 0).astype(F32) + 1.0
    for i in range(owners // 16):
        put_ref[i] = onehot(wide(beside(place, i), RANGE) == number)
    arrived(1)
    arrived(2)

    def place_slots(*accs):
        count = jnp.sum(got_counts[:, 0, :].reshape(owners // 8, 8, 128), axis=1)
        lane = lax.broadcasted_iota(I32, (16, 8, 128), 2)
        row16 = lax.broadcasted_iota(I32, (16, 256), 0)
        for i in range(owners // 16):
            q = i % 2
            put = put_ref[i]
            tiles = got_tiles[16 * i : 16 * i + 16]
            split = jnp.stack([jnp.where(lane < 64, tiles, 0.0), jnp.where(lane < 64, 0.0, tiles)], 1)
            right = jnp.concatenate(two_parts(split.reshape(256, 128)), 1)
            pltpu.matmul_push_rhs(right, staging_register=0, mxu_index=q)
            pltpu.matmul_acc_lhs(accs[q], put, load_staged_rhs=0)
            high, rest = (wide(p.astype(F32), 16) for p in two_parts(beside(count, i)))
            marks = jnp.where(row16 == 0, high, jnp.where(row16 == 1, rest, 0.0)).astype(BF16)
            pltpu.matmul_push_rhs(put, staging_register=1, mxu_index=q, transpose=True)
            pltpu.matmul_acc_lhs(accs[2 + q], marks, load_staged_rhs=1)
        sums = pltpu.matmul_pop(accs[0]) + pltpu.matmul_pop(accs[1])
        counted = pltpu.matmul_pop(accs[2]) + pltpu.matmul_pop(accs[3])
        both = (sums[:, :128] + sums[:, 128:]).T
        ours[0:64] = both[:64] + both[64:]
        ours[64:72] = wide(counted[0:1] + counted[1:2], 8)

    pl.run_scoped(place_slots, *[pltpu.ACC(q)((rows, 256), F32) for rows in (RANGE, 16) for q in range(2)])

    halves = (pl.ds(0, 32), pl.ds(32, 40))
    total = ours[...]
    for step in range(2):
        source = ours if step == 0 else partial
        copies = []
        for n, rows in enumerate(halves):
            copies.append(
                pltpu.make_async_remote_copy(
                    src_ref=source.at[rows], dst_ref=theirs.at[step, rows], send_sem=y_send.at[2 * step + n],
                    recv_sem=y_recv.at[2 * step + n], device_id=(beside_g[(step + n) % 2], me), device_id_type=MESH,
                )
            )
        for copy in copies:
            copy.start()
        for copy in copies:
            copy.wait_recv()
        total = total + theirs[step]
        if step == 0:
            partial[...] = total
        for copy in copies:
            copy.wait_send()
    out_ref[...] = total[0:64] / jnp.maximum(total[64:65], 1.0)


def body(labels, present, values):
    owners, groups = lax.axis_size("dev"), lax.axis_size("grp")
    assert owners == 64 and groups == 4
    times, pixels = values.shape[1:]
    lines = pixels // 128
    return pl.pallas_call(
        functools.partial(fused_kernel, owners),
        out_shape=jax.ShapeDtypeStruct((times, RANGE), F32),
        in_specs=[ANY, ANY, ANY],
        out_specs=VMEM,
        scratch_shapes=[
            pltpu.VMEM((CHUNKS, times, pixels // CHUNKS), BF16),
            pltpu.VMEM((4, 128), I32),
            pltpu.VMEM((lines, 128), I32),
            pltpu.VMEM((lines, 128), F32),
            pltpu.VMEM((lines, 128), F32),
            pltpu.VMEM((8, 128), I32),
            pltpu.VMEM((4, 128), I32),
            pltpu.VMEM((144, 256), F32),
            pltpu.VMEM((owners, 8, 128), F32),
            pltpu.VMEM((owners, 1, 128), F32),
            pltpu.VMEM((owners, 1, 128), F32),
            pltpu.VMEM((owners, 8, 128), F32),
            pltpu.VMEM((owners, 1, 128), F32),
            pltpu.VMEM((owners, 1, 128), F32),
            pltpu.VMEM((owners // 16, RANGE, 256), BF16),
            pltpu.VMEM((72, RANGE), F32),
            pltpu.VMEM((72, RANGE), F32),
            pltpu.VMEM((2, 72, RANGE), F32),
            pltpu.SemaphoreType.DMA((CHUNKS,)),
            pltpu.SemaphoreType.DMA,
            pltpu.SemaphoreType.DMA,
            pltpu.SemaphoreType.DMA((3,)),
            pltpu.SemaphoreType.DMA((3,)),
            pltpu.SemaphoreType.DMA((4,)),
            pltpu.SemaphoreType.DMA((4,)),
        ],
        compiler_params=pltpu.CompilerParams(
            collective_id=0, has_side_effects=True, vmem_limit_bytes=VMEM_LIMIT
        ),
    )(
        pltpu.with_memory_space_constraint(present.reshape(4, 128), pltpu.HBM),
        pltpu.with_memory_space_constraint(labels.reshape(lines, 128), pltpu.HBM),
        pltpu.with_memory_space_constraint(values[0], pltpu.HBM),
    )


def solution(mesh):
    return jax.shard_map(
        body,
        mesh=mesh,
        in_specs=(P(("grp", "dev"), None), P(("grp", "dev"), None), P(("grp", "dev"), None, None)),
        out_specs=P(None, "dev"),
        check_vma=False,
    )
```

```python
import functools

import jax
import jax.numpy as jnp
from jax import lax
from jax.experimental import pallas as pl
from jax.experimental.pallas import tpu as pltpu
from jax.sharding import PartitionSpec as P

ZONES = 16384
RANGE = 256
CAP = 16
CHUNKS = 8
PARTS = 4
F32, BF16, F8, I32 = jnp.float32, jnp.bfloat16, jnp.float8_e4m3fn, jnp.int32
MESH = pl.DeviceIdType.MESH
VMEM = pl.BlockSpec(memory_space=pltpu.VMEM)
ANY = pl.BlockSpec(memory_space=pl.ANY)
VMEM_LIMIT = 48 * 1024 * 1024


def onehot(mask, dtype=BF16):
    return jnp.where(mask, 1.0, 0.0).astype(dtype)


def two_parts(x):
    high = x.astype(BF16)
    return high, (x - high.astype(F32)).astype(BF16)


def lookup(table, word):
    row, lane = word >> 7, word & 127
    out = jnp.zeros_like(word)
    for a in range(8):
        source = jnp.broadcast_to(table[a : a + 1, :], word.shape)
        out = jnp.where(row == a, jnp.take_along_axis(source, lane, axis=1), out)
    return out


def rank_of(labels, table):
    entry = lookup(table, labels >> 4)
    bit = labels & 15
    below = (jnp.full_like(bit, 1) << bit) - 1
    rank = (entry >> 16) + lax.population_count(entry & 65535 & below)
    listed = ((entry >> bit) & 1) == 1
    return rank & 255, jnp.where(listed, rank >> 8, 7)


def wide(row, rows):
    return jnp.broadcast_to(row, (rows, row.shape[1]))


def beside(ref_value, h):
    return jnp.concatenate([ref_value[2 * h : 2 * h + 1], ref_value[2 * h + 1 : 2 * h + 2]], 1)


def make_table(present, accs):
    row8 = lax.broadcasted_iota(I32, (8, 256), 0)
    row128 = lax.broadcasted_iota(I32, (128, 256), 0)
    below = jnp.zeros((8, 1), F32)
    for h in range(2):
        zone = beside(present, h)
        top = wide(zone >> 11, 8)
        middle = wide((zone >> 4) & 127, 128)
        power = (jnp.full_like(zone, 1) << (zone & 15)).astype(F32)
        left = jnp.concatenate(
            [jnp.where(top == row8, wide(power, 8), 0.0), jnp.where(top == row8, 1.0, 0.0)], 0
        ).astype(BF16)
        right = jnp.concatenate([onehot(middle == row128), onehot(middle < row128)], 0)
        pltpu.matmul_push_rhs(right, staging_register=0, mxu_index=h, transpose=True)
        pltpu.matmul_acc_lhs(accs[h], left, load_staged_rhs=0)
        below += jnp.sum(jnp.where(top < row8, 1.0, 0.0), axis=1, keepdims=True)
    both = pltpu.matmul_pop(accs[0]) + pltpu.matmul_pop(accs[1])
    prefix = both[8:16, 128:256] + below
    return (prefix.astype(I32) << 16) | both[0:8, 0:128].astype(I32)


def fused_kernel(
    owners, listed_ref, labels_ref, values_ref, out_ref,
    buf, present_ref, lab_ref, lo_ref, hi_ref, table_ref, slot_ref, sums_ref, tiles_ref, rows_ref,
    got_tiles, got_rows, put_ref, ours, partial, theirs,
    in_sems, listed_sem, lab_sem, send_sems, recv_sems, y_send, y_recv,
):
    g, me = lax.axis_index("grp"), lax.axis_index("dev")
    width = buf.shape[2]
    steps = width // 256
    one, zero = jnp.ones((), BF16), jnp.zeros((), BF16)

    def chunk_copy(k):
        return pltpu.make_async_copy(
            values_ref.at[:, pl.ds(pl.multiple_of(k * width, width), width)], buf.at[k], in_sems.at[k]
        )

    listed_copy = pltpu.make_async_copy(listed_ref, present_ref, listed_sem)
    listed_copy.start()
    lab_copy = pltpu.make_async_copy(labels_ref, lab_ref, lab_sem)
    lab_copy.start()
    barrier = pltpu.get_barrier_semaphore()

    beside_g = (g + 1 - 2 * lax.rem(g, 2), 3 - g)
    for k in range(1, owners):
        if k == 8:
            for n in range(CHUNKS):
                chunk_copy(n).start()
        pl.semaphore_signal(barrier, inc=1, device_id=(g, lax.rem(me + k, owners)), device_id_type=MESH)
    for other in beside_g:
        pl.semaphore_signal(barrier, inc=1, device_id=(other, me), device_id_type=MESH)

    listed_copy.wait()
    present = present_ref[...]
    owner_row = lax.broadcasted_iota(I32, (owners, 256), 0)
    lane_row = lax.broadcasted_iota(I32, (128, 256), 0)
    shift = me // 16 * (2 * CAP)

    def rank_chunk(k):
        rows = pl.ds(pl.multiple_of(k * 64, 64), 64)
        labels = lab_ref[rows, :]
        ranked = [rank_of(labels[8 * i : 8 * i + 8], table_ref[...]) for i in range(8)]
        lo_ref[rows, :] = jnp.concatenate([a for a, _ in ranked], 0).astype(F32)
        hi_ref[rows, :] = jnp.concatenate([b for _, b in ranked], 0).astype(F32)

    def prepare(*accs):
        table = make_table(present, accs[:2])
        first = lookup(table, (present >> 8) << 4) >> 16
        index = lax.broadcasted_iota(I32, present.shape, 0) * 128 + lax.broadcasted_iota(I32, present.shape, 1)
        slot = index - first
        slot_ref[...] = slot
        table_ref[...] = table
        lab_copy.wait()
        rank_chunk(0)

    pl.run_scoped(prepare, *[pltpu.ACC(q)((rows, 256), F32) for rows in (16,) for q in range(2)])

    def send(n, k):
        source, landing = pairs[n]
        to = lax.rem(me + k, owners)
        pltpu.make_async_remote_copy(
            src_ref=source.at[k], dst_ref=landing.at[me], send_sem=send_sems.at[n],
            recv_sem=recv_sems.at[n], device_id=(g, to), device_id_type=MESH,
        ).start()

    pairs = ((rows_ref, got_rows), (tiles_ref, got_tiles))

    def add_up(*refs):
        accs = (refs[:3], refs[3:])
        row256 = lax.broadcasted_iota(I32, (256, 128), 0).astype(F32).astype(BF16)
        row8 = lax.broadcasted_iota(I32, (8, 128), 0).astype(F32)

        def chunk(k):
            chunk_copy(k).wait()
            for j in range(steps):
                q, reg = j % 2, (j // 2) % 2
                hots, first, second, marks = [], [], [], []
                for s in range(2):
                    row = k * (width // 128) + 2 * j + s
                    low = wide(lo_ref[pl.ds(row, 1), :], 16).astype(BF16)
                    high = wide(hi_ref[pl.ds(row, 1), :], 16).astype(BF16)
                    hots.append(jnp.where(jnp.tile(low, (16, 1)) == row256, one, zero).astype(F8))
                    pixels = buf[k, :, pl.ds(256 * j + 128 * s, 128)]
                    high64 = jnp.tile(high, (4, 1))
                    first.append(jnp.where(high64 == zero, pixels, zero))
                    second.append(jnp.where(high64 == one, pixels, zero))
                    marks.append(jnp.where(wide(hi_ref[pl.ds(row, 1), :], 8) == row8, 1.0, 0.0))
                joined = [jnp.concatenate(p, 1) for p in (hots, first, second, marks)]
                pltpu.matmul_push_rhs(joined[0], staging_register=reg, mxu_index=q, transpose=True)
                pltpu.matmul_acc_lhs(accs[q][0], joined[1], load_staged_rhs=reg)
                pltpu.matmul_acc_lhs(accs[q][1], joined[2])
                pltpu.matmul_acc_lhs(accs[q][2], joined[3])

        @pl.loop(0, CHUNKS - 1)
        def _(k):
            chunk(k)
            rank_chunk(k + 1)

        chunk(CHUNKS - 1)
        for a, b, at, rows in zip(accs[0], accs[1], (0, 64, 128), (64, 64, 8)):
            sums_ref[at : at + rows, :] = pltpu.matmul_pop(a) + pltpu.matmul_pop(b)

    pl.run_scoped(add_up, *[pltpu.ACC(q)((rows, 256), F32) for q in range(2) for rows in (64, 64, 8)])

    pl.semaphore_wait(barrier, owners + 1)

    def pick_slots(*accs):
        slot = slot_ref[...]
        part_rows = owners * 8 // PARTS
        pair_row = lax.broadcasted_iota(I32, (part_rows, 256), 0)
        empty = jnp.zeros((64, 256), BF16)
        for h in range(2):
            zone, at = beside(present, h), beside(slot, h)
            mine = wide(((zone >> 8) + (owners - me)) & (owners - 1), owners) == owner_row
            lanes = wide(at, 128) + shift
            lanes = jnp.concatenate([onehot(lanes == lane_row), onehot(lanes + CAP == lane_row)], 0)
            parts = [((zone & 255) + 1).astype(F32)]
            parts += [part.astype(F32) for part in two_parts(sums_ref[128 + h : 129 + h, :])]
            left = jnp.concatenate([jnp.where(mine, wide(part, owners), 0.0) for part in parts], 0)
            pltpu.matmul_push_rhs(lanes, staging_register=0, mxu_index=h, transpose=True)
            pltpu.matmul_acc_lhs(accs[h], left.astype(BF16), load_staged_rhs=0)
        found = pltpu.matmul_pop(accs[0]) + pltpu.matmul_pop(accs[1])
        rows_ref[:, 0, :] = (
            found[:owners, :128] + found[owners : 2 * owners, 128:] + found[2 * owners :, 128:]
        )
        for k in range(1, owners):
            send(0, k)
        for h in range(2):
            zone, at = beside(present, h), beside(slot, h)
            owner = ((zone >> 8) + (owners - me)) & (owners - 1)
            target = ((owner << 3) + (at & 7)) * 2 + (at >> 3)
            high, rest = two_parts(sums_ref[64 * h : 64 * h + 64, :])
            for parity in range(2):
                parts = (high, empty, rest, empty) if parity == 0 else (empty, high, empty, rest)
                pltpu.matmul_push_rhs(
                    jnp.concatenate(parts, 0), staging_register=h, mxu_index=parity, transpose=True
                )
            for part in range(PARTS):
                for parity in range(2):
                    pick = onehot(wide(target, part_rows) == (pair_row + part * part_rows) * 2 + parity)
                    pltpu.matmul_acc_lhs(
                        accs[2 + 2 * part + parity], pick, load_staged_rhs=h if part == 0 else None
                    )
        for part in range(PARTS):
            total = pltpu.matmul_pop(accs[2 + 2 * part]) + pltpu.matmul_pop(accs[3 + 2 * part])
            first = part * owners // PARTS
            tiles_ref[first : first + owners // PARTS] = (total[:, :128] + total[:, 128:]).reshape(-1, 8, 128)
            for k in range(max(first, 1), first + owners // PARTS):
                send(1, k)

    shapes = (owners * 3,) + (owners * 8 // PARTS,) * PARTS
    pl.run_scoped(pick_slots, *[pltpu.ACC(q)((rows, 256), F32) for rows in shapes for q in range(2)])

    for source, landing in pairs:
        landing[me] = source[0]

    def arrived(n):
        source, landing = pairs[n]
        whole = pltpu.make_async_remote_copy(
            src_ref=source.at[pl.ds(0, owners - 1)], dst_ref=landing.at[pl.ds(0, owners - 1)],
            send_sem=send_sems.at[n], recv_sem=recv_sems.at[n],
            device_id=(g, lax.rem(me + 1, owners)), device_id_type=MESH,
        )
        whole.wait_recv()
        whole.wait_send()

    arrived(0)
    rows = got_rows[:, 0, :]
    joined = rows[0:16] + rows[16:32] + rows[32:48] + rows[48:64]
    even = (lax.broadcasted_iota(I32, (8, 128), 1) & CAP) == 0
    place = jnp.where(even, joined[:8], pltpu.roll(joined[8:], CAP, 1))
    count = jnp.where(even, pltpu.roll(joined[:8], 128 - CAP, 1), joined[8:])
    number = lax.broadcasted_iota(I32, (RANGE, 256), 0).astype(F32) + 1.0
    for i in range(owners // 16):
        put_ref[i] = onehot(wide(beside(place, i), RANGE) == number)
    arrived(1)

    def place_slots(*accs):
        lane = lax.broadcasted_iota(I32, (16, 8, 128), 2)
        row16 = lax.broadcasted_iota(I32, (16, 256), 0)
        for i in range(owners // 16):
            q = i % 2
            put = put_ref[i]
            tiles = jnp.stack(
                [got_tiles[16 * a + 8 * b + r] for r in (2 * i, 2 * i + 1) for a in range(4) for b in range(2)], 0
            )
            split = jnp.stack([jnp.where(lane < 64, tiles, 0.0), jnp.where(lane < 64, 0.0, tiles)], 1)
            right = jnp.concatenate(two_parts(split.reshape(256, 128)), 1)
            pltpu.matmul_push_rhs(right, staging_register=0, mxu_index=q)
            pltpu.matmul_acc_lhs(accs[q], put, load_staged_rhs=0)
            high, rest = (wide(p.astype(F32), 16) for p in two_parts(beside(count, i)))
            marks = jnp.where(row16 == 0, high, jnp.where(row16 == 1, rest, 0.0)).astype(BF16)
            pltpu.matmul_push_rhs(put, staging_register=1, mxu_index=q, transpose=True)
            pltpu.matmul_acc_lhs(accs[2 + q], marks, load_staged_rhs=1)
        sums = pltpu.matmul_pop(accs[0]) + pltpu.matmul_pop(accs[1])
        counted = pltpu.matmul_pop(accs[2]) + pltpu.matmul_pop(accs[3])
        both = (sums[:, :128] + sums[:, 128:]).T
        ours[0:64] = both[:64] + both[64:]
        ours[64:72] = wide(counted[0:1] + counted[1:2], 8)

    pl.run_scoped(place_slots, *[pltpu.ACC(q)((rows, 256), F32) for rows in (RANGE, 16) for q in range(2)])

    halves = (pl.ds(0, 32), pl.ds(32, 40))
    total = ours[...]
    for step in range(2):
        source = ours if step == 0 else partial
        copies = []
        for n, rows in enumerate(halves):
            copies.append(
                pltpu.make_async_remote_copy(
                    src_ref=source.at[rows], dst_ref=theirs.at[step, rows], send_sem=y_send.at[2 * step + n],
                    recv_sem=y_recv.at[2 * step + n], device_id=(beside_g[(step + n) % 2], me), device_id_type=MESH,
                )
            )
        for copy in copies:
            copy.start()
        for copy in copies:
            copy.wait_recv()
        total = total + theirs[step]
        if step == 0:
            partial[...] = total
        for copy in copies:
            copy.wait_send()
    out_ref[...] = total[0:64] / jnp.maximum(total[64:65], 1.0)


def body(labels, present, values):
    owners, groups = lax.axis_size("dev"), lax.axis_size("grp")
    assert owners == 64 and groups == 4
    times, pixels = values.shape[1:]
    lines = pixels // 128
    return pl.pallas_call(
        functools.partial(fused_kernel, owners),
        out_shape=jax.ShapeDtypeStruct((times, RANGE), F32),
        in_specs=[ANY, ANY, ANY],
        out_specs=VMEM,
        scratch_shapes=[
            pltpu.VMEM((CHUNKS, times, pixels // CHUNKS), BF16),
            pltpu.VMEM((4, 128), I32),
            pltpu.VMEM((lines, 128), I32),
            pltpu.VMEM((lines, 128), F32),
            pltpu.VMEM((lines, 128), F32),
            pltpu.VMEM((8, 128), I32),
            pltpu.VMEM((4, 128), I32),
            pltpu.VMEM((136, 256), F32),
            pltpu.VMEM((owners, 8, 128), F32),
            pltpu.VMEM((owners, 1, 128), F32),
            pltpu.VMEM((owners, 8, 128), F32),
            pltpu.VMEM((owners, 1, 128), F32),
            pltpu.VMEM((owners // 16, RANGE, 256), BF16),
            pltpu.VMEM((72, RANGE), F32),
            pltpu.VMEM((72, RANGE), F32),
            pltpu.VMEM((2, 72, RANGE), F32),
            pltpu.SemaphoreType.DMA((CHUNKS,)),
            pltpu.SemaphoreType.DMA,
            pltpu.SemaphoreType.DMA,
            pltpu.SemaphoreType.DMA((2,)),
            pltpu.SemaphoreType.DMA((2,)),
            pltpu.SemaphoreType.DMA((4,)),
            pltpu.SemaphoreType.DMA((4,)),
        ],
        compiler_params=pltpu.CompilerParams(
            collective_id=0, has_side_effects=True, vmem_limit_bytes=VMEM_LIMIT
        ),
    )(
        pltpu.with_memory_space_constraint(present.reshape(4, 128), pltpu.HBM),
        pltpu.with_memory_space_constraint(labels.reshape(lines, 128), pltpu.HBM),
        pltpu.with_memory_space_constraint(values[0], pltpu.HBM),
    )


def solution(mesh):
    return jax.shard_map(
        body,
        mesh=mesh,
        in_specs=(P(("grp", "dev"), None), P(("grp", "dev"), None), P(("grp", "dev"), None, None)),
        out_specs=P(None, "dev"),
        check_vma=False,
    )
```

```python
import functools

import jax
import jax.numpy as jnp
from jax import lax
from jax.experimental import pallas as pl
from jax.experimental.pallas import tpu as pltpu
from jax.sharding import PartitionSpec as P

ZONES = 16384
RANGE = 256
CAP = 16
CHUNKS = 8
PARTS = 4
F32, BF16, F8, I32 = jnp.float32, jnp.bfloat16, jnp.float8_e4m3fn, jnp.int32
MESH = pl.DeviceIdType.MESH
VMEM = pl.BlockSpec(memory_space=pltpu.VMEM)
ANY = pl.BlockSpec(memory_space=pl.ANY)
VMEM_LIMIT = 48 * 1024 * 1024


def onehot(mask, dtype=BF16):
    return jnp.where(mask, 1.0, 0.0).astype(dtype)


def two_parts(x):
    high = x.astype(BF16)
    return high, (x - high.astype(F32)).astype(BF16)


def lookup(table, word):
    row, lane = word >> 7, word & 127
    out = jnp.zeros_like(word)
    for a in range(8):
        source = jnp.broadcast_to(table[a : a + 1, :], word.shape)
        out = jnp.where(row == a, jnp.take_along_axis(source, lane, axis=1), out)
    return out


def rank_of(labels, table):
    entry = lookup(table, labels >> 4)
    bit = labels & 15
    below = (jnp.full_like(bit, 1) << bit) - 1
    rank = (entry >> 16) + lax.population_count(entry & 65535 & below)
    listed = ((entry >> bit) & 1) == 1
    return rank & 255, jnp.where(listed, rank >> 8, 7)


def wide(row, rows):
    return jnp.broadcast_to(row, (rows, row.shape[1]))


def beside(ref_value, h):
    return jnp.concatenate([ref_value[2 * h : 2 * h + 1], ref_value[2 * h + 1 : 2 * h + 2]], 1)


def make_table(present, accs):
    row8 = lax.broadcasted_iota(I32, (8, 256), 0)
    row128 = lax.broadcasted_iota(I32, (128, 256), 0)
    below = jnp.zeros((8, 1), F32)
    for h in range(2):
        zone = beside(present, h)
        top = wide(zone >> 11, 8)
        middle = wide((zone >> 4) & 127, 128)
        power = (jnp.full_like(zone, 1) << (zone & 15)).astype(F32)
        left = jnp.concatenate(
            [jnp.where(top == row8, wide(power, 8), 0.0), jnp.where(top == row8, 1.0, 0.0)], 0
        ).astype(BF16)
        right = jnp.concatenate([onehot(middle == row128), onehot(middle < row128)], 0)
        pltpu.matmul_push_rhs(right, staging_register=0, mxu_index=h, transpose=True)
        pltpu.matmul_acc_lhs(accs[h], left, load_staged_rhs=0)
        below += jnp.sum(jnp.where(top < row8, 1.0, 0.0), axis=1, keepdims=True)
    both = pltpu.matmul_pop(accs[0]) + pltpu.matmul_pop(accs[1])
    prefix = both[8:16, 128:256] + below
    return (prefix.astype(I32) << 16) | both[0:8, 0:128].astype(I32)


def fused_kernel(
    owners, listed_ref, labels_ref, values_ref, out_ref,
    buf, present_ref, lab_ref, lo_ref, hi_ref, table_ref, slot_ref, sums_ref, tiles_ref, rows_ref,
    got_tiles, got_rows, put_ref, ours, partial, theirs,
    in_sems, listed_sem, lab_sem, send_sems, recv_sems, y_send, y_recv,
):
    g, me = lax.axis_index("grp"), lax.axis_index("dev")
    width = buf.shape[2]
    steps = width // 256
    one, zero = jnp.ones((), BF16), jnp.zeros((), BF16)

    def chunk_copy(k):
        return pltpu.make_async_copy(
            values_ref.at[:, pl.ds(pl.multiple_of(k * width, width), width)], buf.at[k], in_sems.at[k]
        )

    listed_copy = pltpu.make_async_copy(listed_ref, present_ref, listed_sem)
    listed_copy.start()
    lab_copy = pltpu.make_async_copy(labels_ref, lab_ref, lab_sem)
    lab_copy.start()
    barrier = pltpu.get_barrier_semaphore()

    beside_g = (g + 1 - 2 * lax.rem(g, 2), 3 - g)
    for k in range(1, owners):
        if k == 8:
            for n in range(CHUNKS):
                chunk_copy(n).start()
        pl.semaphore_signal(barrier, inc=1, device_id=(g, lax.rem(me + k, owners)), device_id_type=MESH)
    for other in beside_g:
        pl.semaphore_signal(barrier, inc=1, device_id=(other, me), device_id_type=MESH)

    listed_copy.wait()
    present = present_ref[...]
    owner_row = lax.broadcasted_iota(I32, (owners, 256), 0)
    lane_row = lax.broadcasted_iota(I32, (128, 256), 0)
    shift = me // 16 * (2 * CAP)

    def rank_chunk(k):
        rows = pl.ds(pl.multiple_of(k * 64, 64), 64)
        labels = lab_ref[rows, :]
        ranked = [rank_of(labels[8 * i : 8 * i + 8], table_ref[...]) for i in range(8)]
        lo_ref[rows, :] = jnp.concatenate([a for a, _ in ranked], 0).astype(F32)
        hi_ref[rows, :] = jnp.concatenate([b for _, b in ranked], 0).astype(F32)

    def prepare(*accs):
        table = make_table(present, accs[:2])
        first = lookup(table, (present >> 8) << 4) >> 16
        index = lax.broadcasted_iota(I32, present.shape, 0) * 128 + lax.broadcasted_iota(I32, present.shape, 1)
        slot = index - first
        slot_ref[...] = slot
        table_ref[...] = table
        lab_copy.wait()
        rank_chunk(0)

    pl.run_scoped(prepare, *[pltpu.ACC(q)((rows, 256), F32) for rows in (16,) for q in range(2)])

    def send(n, k):
        source, landing = pairs[n]
        to = lax.rem(me + k, owners)
        pltpu.make_async_remote_copy(
            src_ref=source.at[k], dst_ref=landing.at[me], send_sem=send_sems.at[n],
            recv_sem=recv_sems.at[n], device_id=(g, to), device_id_type=MESH,
        ).start()

    pairs = ((rows_ref, got_rows), (tiles_ref, got_tiles))

    def add_up(*refs):
        accs = (refs[:3], refs[3:])
        row256 = lax.broadcasted_iota(I32, (256, 128), 0).astype(F32).astype(BF16)
        row8 = lax.broadcasted_iota(I32, (8, 128), 0).astype(F32)

        def chunk(k):
            chunk_copy(k).wait()
            for j in range(steps):
                q, reg = j % 2, (j // 2) % 2
                hots, first, second, marks = [], [], [], []
                for s in range(2):
                    row = k * (width // 128) + 2 * j + s
                    low = wide(lo_ref[pl.ds(row, 1), :], 16).astype(BF16)
                    high = wide(hi_ref[pl.ds(row, 1), :], 16).astype(BF16)
                    hots.append(jnp.where(jnp.tile(low, (16, 1)) == row256, one, zero).astype(F8))
                    pixels = buf[k, :, pl.ds(256 * j + 128 * s, 128)]
                    high64 = jnp.tile(high, (4, 1))
                    first.append(jnp.where(high64 == zero, pixels, zero))
                    second.append(jnp.where(high64 == one, pixels, zero))
                    marks.append(jnp.where(wide(hi_ref[pl.ds(row, 1), :], 8) == row8, 1.0, 0.0))
                joined = [jnp.concatenate(p, 1) for p in (hots, first, second, marks)]
                pltpu.matmul_push_rhs(joined[0], staging_register=reg, mxu_index=q, transpose=True)
                pltpu.matmul_acc_lhs(accs[q][0], joined[1], load_staged_rhs=reg)
                pltpu.matmul_acc_lhs(accs[q][1], joined[2])
                pltpu.matmul_acc_lhs(accs[q][2], joined[3])

        @pl.loop(0, CHUNKS - 1)
        def _(k):
            chunk(k)
            rank_chunk(k + 1)

        chunk(CHUNKS - 1)
        for a, b, at, rows in zip(accs[0], accs[1], (0, 64, 128), (64, 64, 8)):
            sums_ref[at : at + rows, :] = pltpu.matmul_pop(a) + pltpu.matmul_pop(b)

    pl.run_scoped(add_up, *[pltpu.ACC(q)((rows, 256), F32) for q in range(2) for rows in (64, 64, 8)])

    pl.semaphore_wait(barrier, owners + 1)

    def pick_slots(*accs):
        slot = slot_ref[...]
        part_rows = owners * 8 // PARTS
        pair_row = lax.broadcasted_iota(I32, (part_rows, 256), 0)
        empty = jnp.zeros((64, 256), BF16)
        for h in range(2):
            zone, at = beside(present, h), beside(slot, h)
            mine = wide(((zone >> 8) + (owners - me)) & (owners - 1), owners) == owner_row
            lanes = wide(at, 128) + shift
            lanes = jnp.concatenate([onehot(lanes == lane_row), onehot(lanes + CAP == lane_row)], 0)
            parts = [((zone & 255) + 1).astype(F32)]
            parts += [part.astype(F32) for part in two_parts(sums_ref[128 + h : 129 + h, :])]
            left = jnp.concatenate([jnp.where(mine, wide(part, owners), 0.0) for part in parts], 0)
            pltpu.matmul_push_rhs(lanes, staging_register=0, mxu_index=h, transpose=True)
            pltpu.matmul_acc_lhs(accs[h], left.astype(BF16), load_staged_rhs=0)
        found = pltpu.matmul_pop(accs[0]) + pltpu.matmul_pop(accs[1])
        rows_ref[:, 0, :] = (
            found[:owners, :128] + found[owners : 2 * owners, 128:] + found[2 * owners :, 128:]
        )
        for k in range(1, owners):
            send(0, k)
        for h in range(2):
            zone, at = beside(present, h), beside(slot, h)
            owner = ((zone >> 8) + (owners - me)) & (owners - 1)
            target = ((owner << 3) + (at & 7)) * 2 + (at >> 3)
            high, rest = two_parts(sums_ref[64 * h : 64 * h + 64, :])
            for parity in range(2):
                parts = (high, empty, rest, empty) if parity == 0 else (empty, high, empty, rest)
                pltpu.matmul_push_rhs(
                    jnp.concatenate(parts, 0), staging_register=h, mxu_index=parity, transpose=True
                )
            for part in range(PARTS):
                for parity in range(2):
                    pick = onehot(wide(target, part_rows) == (pair_row + part * part_rows) * 2 + parity)
                    pltpu.matmul_acc_lhs(
                        accs[2 + 2 * part + parity], pick, load_staged_rhs=h if part == 0 else None
                    )
        for part in range(PARTS):
            total = pltpu.matmul_pop(accs[2 + 2 * part]) + pltpu.matmul_pop(accs[3 + 2 * part])
            first = part * owners // PARTS
            tiles_ref[first : first + owners // PARTS] = (total[:, :128] + total[:, 128:]).reshape(-1, 8, 128)
            for k in range(max(first, 1), first + owners // PARTS):
                send(1, k)

    shapes = (owners * 3,) + (owners * 8 // PARTS,) * PARTS
    pl.run_scoped(pick_slots, *[pltpu.ACC(q)((rows, 256), F32) for rows in shapes for q in range(2)])

    for source, landing in pairs:
        landing[me] = source[0]

    def arrived(n):
        source, landing = pairs[n]
        whole = pltpu.make_async_remote_copy(
            src_ref=source.at[pl.ds(0, owners - 1)], dst_ref=landing.at[pl.ds(0, owners - 1)],
            send_sem=send_sems.at[n], recv_sem=recv_sems.at[n],
            device_id=(g, lax.rem(me + 1, owners)), device_id_type=MESH,
        )
        whole.wait_recv()
        whole.wait_send()

    arrived(0)
    rows = got_rows[:, 0, :]
    joined = rows[0:16] + rows[16:32] + rows[32:48] + rows[48:64]
    even = (lax.broadcasted_iota(I32, (8, 128), 1) & CAP) == 0
    place = jnp.where(even, joined[:8], pltpu.roll(joined[8:], CAP, 1))
    count = jnp.where(even, pltpu.roll(joined[:8], 128 - CAP, 1), joined[8:])
    number = lax.broadcasted_iota(I32, (RANGE, 256), 0).astype(F32) + 1.0
    for i in range(owners // 16):
        put_ref[i] = onehot(wide(beside(place, i), RANGE) == number)
    arrived(1)

    def place_slots(*accs):
        lane = lax.broadcasted_iota(I32, (16, 8, 128), 2)
        row16 = lax.broadcasted_iota(I32, (16, 256), 0)
        for i in range(owners // 16):
            q = i % 2
            put = put_ref[i]
            tiles = jnp.stack(
                [got_tiles[16 * a + 8 * b + r] for r in (2 * i, 2 * i + 1) for a in range(4) for b in range(2)], 0
            )
            split = jnp.stack([jnp.where(lane < 64, tiles, 0.0), jnp.where(lane < 64, 0.0, tiles)], 1)
            right = jnp.concatenate(two_parts(split.reshape(256, 128)), 1)
            pltpu.matmul_push_rhs(right, staging_register=0, mxu_index=q)
            pltpu.matmul_acc_lhs(accs[q], put, load_staged_rhs=0)
            high, rest = (wide(p.astype(F32), 16) for p in two_parts(beside(count, i)))
            marks = jnp.where(row16 == 0, high, jnp.where(row16 == 1, rest, 0.0)).astype(BF16)
            pltpu.matmul_push_rhs(put, staging_register=1, mxu_index=q, transpose=True)
            pltpu.matmul_acc_lhs(accs[2 + q], marks, load_staged_rhs=1)
        sums = pltpu.matmul_pop(accs[0]) + pltpu.matmul_pop(accs[1])
        counted = pltpu.matmul_pop(accs[2]) + pltpu.matmul_pop(accs[3])
        both = (sums[:, :128] + sums[:, 128:]).T
        ours[0:64] = both[:64] + both[64:]
        ours[64:72] = wide(counted[0:1] + counted[1:2], 8)

    pl.run_scoped(place_slots, *[pltpu.ACC(q)((rows, 256), F32) for rows in (RANGE, 16) for q in range(2)])

    pieces = ((48, 24, 1), (0, 16, 0), (32, 16, 1), (16, 16, 0))

    def y_copy(step, n):
        at, rows, turn = pieces[n]
        source = ours if step == 0 else partial
        return pltpu.make_async_remote_copy(
            src_ref=source.at[pl.ds(at, rows)], dst_ref=theirs.at[step, pl.ds(at, rows)],
            send_sem=y_send.at[4 * step + n], recv_sem=y_recv.at[4 * step + n],
            device_id=(beside_g[(step + turn) % 2], me), device_id_type=MESH,
        )

    for n in range(4):
        y_copy(0, n).start()
    for n, (at, rows, _) in enumerate(pieces):
        y_copy(0, n).wait_recv()
        partial[at : at + rows] = ours[at : at + rows] + theirs[0, at : at + rows]
        y_copy(1, n).start()
    counts = None
    for n, (at, rows, _) in enumerate(pieces):
        y_copy(1, n).wait_recv()
        total = partial[at : at + rows] + theirs[1, at : at + rows]
        if n == 0:
            counts = jnp.maximum(total[16:17], 1.0)
            total = total[:16]
        out_ref[at : at + 16] = total / counts
    for step in range(2):
        for n in range(4):
            y_copy(step, n).wait_send()


def body(labels, present, values):
    owners, groups = lax.axis_size("dev"), lax.axis_size("grp")
    assert owners == 64 and groups == 4
    times, pixels = values.shape[1:]
    lines = pixels // 128
    return pl.pallas_call(
        functools.partial(fused_kernel, owners),
        out_shape=jax.ShapeDtypeStruct((times, RANGE), F32),
        in_specs=[ANY, ANY, ANY],
        out_specs=VMEM,
        scratch_shapes=[
            pltpu.VMEM((CHUNKS, times, pixels // CHUNKS), BF16),
            pltpu.VMEM((4, 128), I32),
            pltpu.VMEM((lines, 128), I32),
            pltpu.VMEM((lines, 128), F32),
            pltpu.VMEM((lines, 128), F32),
            pltpu.VMEM((8, 128), I32),
            pltpu.VMEM((4, 128), I32),
            pltpu.VMEM((136, 256), F32),
            pltpu.VMEM((owners, 8, 128), F32),
            pltpu.VMEM((owners, 1, 128), F32),
            pltpu.VMEM((owners, 8, 128), F32),
            pltpu.VMEM((owners, 1, 128), F32),
            pltpu.VMEM((owners // 16, RANGE, 256), BF16),
            pltpu.VMEM((72, RANGE), F32),
            pltpu.VMEM((72, RANGE), F32),
            pltpu.VMEM((2, 72, RANGE), F32),
            pltpu.SemaphoreType.DMA((CHUNKS,)),
            pltpu.SemaphoreType.DMA,
            pltpu.SemaphoreType.DMA,
            pltpu.SemaphoreType.DMA((2,)),
            pltpu.SemaphoreType.DMA((2,)),
            pltpu.SemaphoreType.DMA((8,)),
            pltpu.SemaphoreType.DMA((8,)),
        ],
        compiler_params=pltpu.CompilerParams(
            collective_id=0, has_side_effects=True, vmem_limit_bytes=VMEM_LIMIT
        ),
    )(
        pltpu.with_memory_space_constraint(present.reshape(4, 128), pltpu.HBM),
        pltpu.with_memory_space_constraint(labels.reshape(lines, 128), pltpu.HBM),
        pltpu.with_memory_space_constraint(values[0], pltpu.HBM),
    )


def solution(mesh):
    return jax.shard_map(
        body,
        mesh=mesh,
        in_specs=(P(("grp", "dev"), None), P(("grp", "dev"), None), P(("grp", "dev"), None, None)),
        out_specs=P(None, "dev"),
        check_vma=False,
    )
```

```python
import functools

import jax
import jax.numpy as jnp
from jax import lax
from jax.experimental import pallas as pl
from jax.experimental.pallas import tpu as pltpu
from jax.sharding import PartitionSpec as P

ZONES = 16384
RANGE = 256
CAP = 16
CHUNKS = 8
PARTS = 4
F32, BF16, F8, I32 = jnp.float32, jnp.bfloat16, jnp.float8_e4m3fn, jnp.int32
MESH = pl.DeviceIdType.MESH
VMEM = pl.BlockSpec(memory_space=pltpu.VMEM)
ANY = pl.BlockSpec(memory_space=pl.ANY)
VMEM_LIMIT = 48 * 1024 * 1024


def onehot(mask, dtype=BF16):
    return jnp.where(mask, 1.0, 0.0).astype(dtype)


def two_parts(x):
    high = x.astype(BF16)
    return high, (x - high.astype(F32)).astype(BF16)


def lookup(table, word):
    row, lane = word >> 7, word & 127
    out = jnp.zeros_like(word)
    for a in range(8):
        source = jnp.broadcast_to(table[a : a + 1, :], word.shape)
        out = jnp.where(row == a, jnp.take_along_axis(source, lane, axis=1), out)
    return out


def rank_of(labels, table):
    entry = lookup(table, labels >> 4)
    bit = labels & 15
    below = (jnp.full_like(bit, 1) << bit) - 1
    rank = (entry >> 16) + lax.population_count(entry & 65535 & below)
    listed = ((entry >> bit) & 1) == 1
    return rank & 255, jnp.where(listed, rank >> 8, 7)


def wide(row, rows):
    return jnp.broadcast_to(row, (rows, row.shape[1]))


def beside(ref_value, h):
    return jnp.concatenate([ref_value[2 * h : 2 * h + 1], ref_value[2 * h + 1 : 2 * h + 2]], 1)


def make_table(present, accs):
    row8 = lax.broadcasted_iota(I32, (8, 256), 0)
    row128 = lax.broadcasted_iota(I32, (128, 256), 0)
    below = jnp.zeros((8, 1), F32)
    for h in range(2):
        zone = beside(present, h)
        top = wide(zone >> 11, 8)
        middle = wide((zone >> 4) & 127, 128)
        power = (jnp.full_like(zone, 1) << (zone & 15)).astype(F32)
        left = jnp.concatenate(
            [jnp.where(top == row8, wide(power, 8), 0.0), jnp.where(top == row8, 1.0, 0.0)], 0
        ).astype(BF16)
        right = jnp.concatenate([onehot(middle == row128), onehot(middle < row128)], 0)
        pltpu.matmul_push_rhs(right, staging_register=0, mxu_index=h, transpose=True)
        pltpu.matmul_acc_lhs(accs[h], left, load_staged_rhs=0)
        below += jnp.sum(jnp.where(top < row8, 1.0, 0.0), axis=1, keepdims=True)
    both = pltpu.matmul_pop(accs[0]) + pltpu.matmul_pop(accs[1])
    prefix = both[8:16, 128:256] + below
    return (prefix.astype(I32) << 16) | both[0:8, 0:128].astype(I32)


def fused_kernel(
    owners, listed_ref, labels_ref, values_ref, out_ref,
    buf, present_ref, lab_ref, lo_ref, hi_ref, table_ref, slot_ref, sums_ref, tiles_ref, rows_ref,
    got_tiles, got_rows, put_ref, ours, partial, theirs,
    in_sems, listed_sem, lab_sem, send_sems, recv_sems, y_send, y_recv,
):
    g, me = lax.axis_index("grp"), lax.axis_index("dev")
    width = buf.shape[2]
    steps = width // 256
    one, zero = jnp.ones((), BF16), jnp.zeros((), BF16)

    def chunk_copy(k):
        return pltpu.make_async_copy(
            values_ref.at[:, pl.ds(pl.multiple_of(k * width, width), width)], buf.at[k], in_sems.at[k]
        )

    listed_copy = pltpu.make_async_copy(listed_ref, present_ref, listed_sem)
    listed_copy.start()
    lab_copy = pltpu.make_async_copy(labels_ref, lab_ref, lab_sem)
    lab_copy.start()
    barrier = pltpu.get_barrier_semaphore()

    beside_g = (g + 1 - 2 * lax.rem(g, 2), 3 - g)
    for k in range(1, owners):
        if k == 8:
            for n in range(CHUNKS):
                chunk_copy(n).start()
        pl.semaphore_signal(barrier, inc=1, device_id=(g, lax.rem(me + k, owners)), device_id_type=MESH)
    for other in beside_g:
        pl.semaphore_signal(barrier, inc=1, device_id=(other, me), device_id_type=MESH)

    listed_copy.wait()
    present = present_ref[...]
    owner_row = lax.broadcasted_iota(I32, (owners, 256), 0)
    lane_row = lax.broadcasted_iota(I32, (128, 256), 0)
    shift = me // 16 * (2 * CAP)

    def rank_chunk(k):
        rows = pl.ds(pl.multiple_of(k * 64, 64), 64)
        labels = lab_ref[rows, :]
        ranked = [rank_of(labels[8 * i : 8 * i + 8], table_ref[...]) for i in range(8)]
        lo_ref[rows, :] = jnp.concatenate([a for a, _ in ranked], 0).astype(F32)
        hi_ref[rows, :] = jnp.concatenate([b for _, b in ranked], 0).astype(F32)

    def prepare(*accs):
        table = make_table(present, accs[:2])
        first = lookup(table, (present >> 8) << 4) >> 16
        index = lax.broadcasted_iota(I32, present.shape, 0) * 128 + lax.broadcasted_iota(I32, present.shape, 1)
        slot = index - first
        slot_ref[...] = slot
        table_ref[...] = table
        lab_copy.wait()
        rank_chunk(0)

    pl.run_scoped(prepare, *[pltpu.ACC(q)((rows, 256), F32) for rows in (16,) for q in range(2)])

    def send(n, k):
        source, landing = pairs[n]
        to = lax.rem(me + k, owners)
        pltpu.make_async_remote_copy(
            src_ref=source.at[k], dst_ref=landing.at[me], send_sem=send_sems.at[n],
            recv_sem=recv_sems.at[n], device_id=(g, to), device_id_type=MESH,
        ).start()

    pairs = ((rows_ref, got_rows), (tiles_ref, got_tiles))

    def add_up(*refs):
        accs = (refs[:3], refs[3:])
        row256 = lax.broadcasted_iota(I32, (256, 128), 0).astype(F32).astype(BF16)
        row8 = lax.broadcasted_iota(I32, (8, 128), 0).astype(F32)

        def chunk(k):
            chunk_copy(k).wait()
            for j in range(steps):
                q, reg = j % 2, (j // 2) % 2
                hots, first, second, marks = [], [], [], []
                for s in range(2):
                    row = k * (width // 128) + 2 * j + s
                    low = wide(lo_ref[pl.ds(row, 1), :], 16).astype(BF16)
                    high = wide(hi_ref[pl.ds(row, 1), :], 16).astype(BF16)
                    hots.append(jnp.where(jnp.tile(low, (16, 1)) == row256, one, zero).astype(F8))
                    pixels = buf[k, :, pl.ds(256 * j + 128 * s, 128)]
                    high64 = jnp.tile(high, (4, 1))
                    first.append(jnp.where(high64 == zero, pixels, zero))
                    second.append(jnp.where(high64 == one, pixels, zero))
                    marks.append(jnp.where(wide(hi_ref[pl.ds(row, 1), :], 8) == row8, 1.0, 0.0))
                joined = [jnp.concatenate(p, 1) for p in (hots, first, second, marks)]
                pltpu.matmul_push_rhs(joined[0], staging_register=reg, mxu_index=q, transpose=True)
                pltpu.matmul_acc_lhs(accs[q][0], joined[1], load_staged_rhs=reg)
                pltpu.matmul_acc_lhs(accs[q][1], joined[2])
                pltpu.matmul_acc_lhs(accs[q][2], joined[3])

        @pl.loop(0, CHUNKS - 1)
        def _(k):
            chunk(k)
            rank_chunk(k + 1)

        chunk(CHUNKS - 1)
        for a, b, at, rows in zip(accs[0], accs[1], (0, 64, 128), (64, 64, 8)):
            sums_ref[at : at + rows, :] = pltpu.matmul_pop(a) + pltpu.matmul_pop(b)

    pl.run_scoped(add_up, *[pltpu.ACC(q)((rows, 256), F32) for q in range(2) for rows in (64, 64, 8)])

    pl.semaphore_wait(barrier, owners + 1)

    def pick_slots(*accs):
        slot = slot_ref[...]
        part_rows = owners * 8 // PARTS
        pair_row = lax.broadcasted_iota(I32, (part_rows, 256), 0)
        empty = jnp.zeros((64, 256), BF16)
        for h in range(2):
            zone, at = beside(present, h), beside(slot, h)
            mine = wide(((zone >> 8) + (owners - me)) & (owners - 1), owners) == owner_row
            lanes = wide(at, 128) + shift
            lanes = jnp.concatenate([onehot(lanes == lane_row), onehot(lanes + CAP == lane_row)], 0)
            parts = [((zone & 255) + 1).astype(F32)]
            parts += [part.astype(F32) for part in two_parts(sums_ref[128 + h : 129 + h, :])]
            left = jnp.concatenate([jnp.where(mine, wide(part, owners), 0.0) for part in parts], 0)
            pltpu.matmul_push_rhs(lanes, staging_register=0, mxu_index=h, transpose=True)
            pltpu.matmul_acc_lhs(accs[h], left.astype(BF16), load_staged_rhs=0)
        found = pltpu.matmul_pop(accs[0]) + pltpu.matmul_pop(accs[1])
        rows_ref[:, 0, :] = (
            found[:owners, :128] + found[owners : 2 * owners, 128:] + found[2 * owners :, 128:]
        )
        for k in range(1, owners):
            send(0, k)
        for h in range(2):
            zone, at = beside(present, h), beside(slot, h)
            owner = ((zone >> 8) + (owners - me)) & (owners - 1)
            target = ((owner << 3) + (at & 7)) * 2 + (at >> 3)
            high, rest = two_parts(sums_ref[64 * h : 64 * h + 64, :])
            for parity in range(2):
                parts = (high, empty, rest, empty) if parity == 0 else (empty, high, empty, rest)
                pltpu.matmul_push_rhs(
                    jnp.concatenate(parts, 0), staging_register=h, mxu_index=parity, transpose=True
                )
            for part in range(PARTS):
                for parity in range(2):
                    pick = onehot(wide(target, part_rows) == (pair_row + part * part_rows) * 2 + parity)
                    pltpu.matmul_acc_lhs(
                        accs[2 + 2 * part + parity], pick, load_staged_rhs=h if part == 0 else None
                    )
        for part in range(PARTS):
            total = pltpu.matmul_pop(accs[2 + 2 * part]) + pltpu.matmul_pop(accs[3 + 2 * part])
            first = part * owners // PARTS
            tiles_ref[first : first + owners // PARTS] = (total[:, :128] + total[:, 128:]).reshape(-1, 8, 128)
            for k in range(max(first, 1), first + owners // PARTS):
                send(1, k)

    shapes = (owners * 3,) + (owners * 8 // PARTS,) * PARTS
    pl.run_scoped(pick_slots, *[pltpu.ACC(q)((rows, 256), F32) for rows in shapes for q in range(2)])

    for source, landing in pairs:
        landing[me] = source[0]

    def whole(n):
        source, landing = pairs[n]
        return pltpu.make_async_remote_copy(
            src_ref=source.at[pl.ds(0, owners - 1)], dst_ref=landing.at[pl.ds(0, owners - 1)],
            send_sem=send_sems.at[n], recv_sem=recv_sems.at[n],
            device_id=(g, lax.rem(me + 1, owners)), device_id_type=MESH,
        )

    whole(0).wait_recv()
    rows = got_rows[:, 0, :]
    joined = rows[0:16] + rows[16:32] + rows[32:48] + rows[48:64]
    even = (lax.broadcasted_iota(I32, (8, 128), 1) & CAP) == 0
    place = jnp.where(even, joined[:8], pltpu.roll(joined[8:], CAP, 1))
    count = jnp.where(even, pltpu.roll(joined[:8], 128 - CAP, 1), joined[8:])
    number = lax.broadcasted_iota(I32, (RANGE, 256), 0).astype(F32) + 1.0
    for i in range(owners // 16):
        put_ref[i] = onehot(wide(beside(place, i), RANGE) == number)
    whole(1).wait_recv()

    def place_slots(*accs):
        lane = lax.broadcasted_iota(I32, (16, 8, 128), 2)
        row16 = lax.broadcasted_iota(I32, (16, 256), 0)
        for i in range(owners // 16):
            q = i % 2
            put = put_ref[i]
            tiles = jnp.stack(
                [got_tiles[16 * a + 8 * b + r] for r in (2 * i, 2 * i + 1) for a in range(4) for b in range(2)], 0
            )
            split = jnp.stack([jnp.where(lane < 64, tiles, 0.0), jnp.where(lane < 64, 0.0, tiles)], 1)
            right = jnp.concatenate(two_parts(split.reshape(256, 128)), 1)
            pltpu.matmul_push_rhs(right, staging_register=0, mxu_index=q)
            pltpu.matmul_acc_lhs(accs[q], put, load_staged_rhs=0)
            high, rest = (wide(p.astype(F32), 16) for p in two_parts(beside(count, i)))
            marks = jnp.where(row16 == 0, high, jnp.where(row16 == 1, rest, 0.0)).astype(BF16)
            pltpu.matmul_push_rhs(put, staging_register=1, mxu_index=q, transpose=True)
            pltpu.matmul_acc_lhs(accs[2 + q], marks, load_staged_rhs=1)
        sums = pltpu.matmul_pop(accs[0]) + pltpu.matmul_pop(accs[1])
        counted = pltpu.matmul_pop(accs[2]) + pltpu.matmul_pop(accs[3])
        both = (sums[:, :128] + sums[:, 128:]).T
        ours[0:64] = both[:64] + both[64:]
        ours[64:72] = wide(counted[0:1] + counted[1:2], 8)

    pl.run_scoped(place_slots, *[pltpu.ACC(q)((rows, 256), F32) for rows in (RANGE, 16) for q in range(2)])

    pieces = ((48, 24, 1), (0, 16, 0), (32, 16, 1), (16, 16, 0))

    def y_copy(step, n):
        at, rows, turn = pieces[n]
        source = ours if step == 0 else partial
        return pltpu.make_async_remote_copy(
            src_ref=source.at[pl.ds(at, rows)], dst_ref=theirs.at[step, pl.ds(at, rows)],
            send_sem=y_send.at[4 * step + n], recv_sem=y_recv.at[4 * step + n],
            device_id=(beside_g[(step + turn) % 2], me), device_id_type=MESH,
        )

    for n in range(4):
        y_copy(0, n).start()
    for n, (at, rows, _) in enumerate(pieces):
        y_copy(0, n).wait_recv()
        partial[at : at + rows] = ours[at : at + rows] + theirs[0, at : at + rows]
        y_copy(1, n).start()
    counts = None
    for n, (at, rows, _) in enumerate(pieces):
        y_copy(1, n).wait_recv()
        total = partial[at : at + rows] + theirs[1, at : at + rows]
        if n == 0:
            counts = jnp.maximum(total[16:17], 1.0)
            total = total[:16]
        out_ref[at : at + 16] = total / counts
    for n in range(2):
        whole(n).wait_send()
    for step in range(2):
        for n in range(4):
            y_copy(step, n).wait_send()


def body(labels, present, values):
    owners, groups = lax.axis_size("dev"), lax.axis_size("grp")
    assert owners == 64 and groups == 4
    times, pixels = values.shape[1:]
    lines = pixels // 128
    return pl.pallas_call(
        functools.partial(fused_kernel, owners),
        out_shape=jax.ShapeDtypeStruct((times, RANGE), F32),
        in_specs=[ANY, ANY, ANY],
        out_specs=VMEM,
        scratch_shapes=[
            pltpu.VMEM((CHUNKS, times, pixels // CHUNKS), BF16),
            pltpu.VMEM((4, 128), I32),
            pltpu.VMEM((lines, 128), I32),
            pltpu.VMEM((lines, 128), F32),
            pltpu.VMEM((lines, 128), F32),
            pltpu.VMEM((8, 128), I32),
            pltpu.VMEM((4, 128), I32),
            pltpu.VMEM((136, 256), F32),
            pltpu.VMEM((owners, 8, 128), F32),
            pltpu.VMEM((owners, 1, 128), F32),
            pltpu.VMEM((owners, 8, 128), F32),
            pltpu.VMEM((owners, 1, 128), F32),
            pltpu.VMEM((owners // 16, RANGE, 256), BF16),
            pltpu.VMEM((72, RANGE), F32),
            pltpu.VMEM((72, RANGE), F32),
            pltpu.VMEM((2, 72, RANGE), F32),
            pltpu.SemaphoreType.DMA((CHUNKS,)),
            pltpu.SemaphoreType.DMA,
            pltpu.SemaphoreType.DMA,
            pltpu.SemaphoreType.DMA((2,)),
            pltpu.SemaphoreType.DMA((2,)),
            pltpu.SemaphoreType.DMA((8,)),
            pltpu.SemaphoreType.DMA((8,)),
        ],
        compiler_params=pltpu.CompilerParams(
            collective_id=0, has_side_effects=True, vmem_limit_bytes=VMEM_LIMIT
        ),
    )(
        pltpu.with_memory_space_constraint(present.reshape(4, 128), pltpu.HBM),
        pltpu.with_memory_space_constraint(labels.reshape(lines, 128), pltpu.HBM),
        pltpu.with_memory_space_constraint(values[0], pltpu.HBM),
    )


def solution(mesh):
    return jax.shard_map(
        body,
        mesh=mesh,
        in_specs=(P(("grp", "dev"), None), P(("grp", "dev"), None), P(("grp", "dev"), None, None)),
        out_specs=P(None, "dev"),
        check_vma=False,
    )
```
